256 devices in a mesh: dp: 8 (over y_hi, x), ctx: 32 (over z, y_lo, core).
Axes of the slice: x: 4, y: 4 (y_hi: 2, y_lo: 2; y = y_hi * 2 + y_lo), z: 8, core: 2. Of those that a mesh axis runs over, the one named last changes fastest.
Arguments:
- layer_input: bfloat16 [8, 4096, 7168], P(None, 'ctx', 'dp'), may hold values from -6 to 6
- kv_latent: bfloat16 [8, 4096, 512], P('dp', 'ctx'), may hold values from -8 to 8
- key_rope: bfloat16 [8, 4096, 64], P('dp', 'ctx'), may hold values from -6 to 6
- q_latent: bfloat16 [8, 4096, 8, 512], P('dp', 'ctx'), may hold values from -60 to 60
- q_rope: bfloat16 [8, 4096, 8, 64], P('dp', 'ctx'), may hold values from -3 to 3
- saved_output: bfloat16 [8, 4096, 8, 512], P('dp', 'ctx'), may hold values from -4 to 4
- w_uv: bfloat16 [512, 1024], replicated, may hold values from -0.25 to 0.25
- d_out: bfloat16 [8, 4096, 1024], P('dp', 'ctx'), may hold values from -6 to 6
- blocks: int32 [64], replicated, may hold values from 0 to 63, each once
Outputs:
- d_q_latent: bfloat16 [8, 4096, 8, 512], P('dp', 'ctx')
- d_q_rope: bfloat16 [8, 4096, 8, 64], P('dp', 'ctx')
- d_kv_latent: bfloat16 [8, 4096, 512], P('dp', 'ctx')
- d_key_rope: bfloat16 [8, 4096, 64], P('dp', 'ctx')
- grad_w_down: float32 [7168, 576], P(('dp', 'ctx'))
- grad_w_uv: float32 [512, 1024], P(('dp', 'ctx'))
The draws below stay inside these ranges and needn't reach their ends.
Inputs may be any that keep to these rules, and one draw needn't show every extreme that they name: A permutation: blocks[k] is the position block of rows k * 64 to (k + 1) * 64 - 1 of every sequence.
All inputs are finite; a program needn't handle non-finite values.
Results may differ from the reference program's by a relative error of at most 0.028.
Values may be sent and summed in bfloat16 or wider, within the bound.
No kernel may reach another device: no remote copies, remote signals or barrier semaphores. Data moves between devices by JAX's collectives and lax.ppermute only.
A program may use at most 128 MiB of HBM per device.

```python
import functools
import math
import jax
import jax.numpy as jnp
from jax import lax

D = 7168
KVL = 512
ROPE = 64
VHEAD = 128
HEADS = 8
TOK_DEV = 128
SEQ = 4096
N_DP = 8
N_CTX = 32


def base_latent(key):
    return jnp.clip(jax.random.normal(jax.random.fold_in(key, 7), (N_DP, SEQ, KVL), jnp.float32), -6.0, 6.0)


def draw_kv_latent(key, part):
    latent = base_latent(key)
    return latent.astype(jnp.bfloat16)


def draw_q_latent(key, part):
    queries = 0.5 * jnp.clip(jax.random.normal(jax.random.fold_in(key, 9), (N_DP, SEQ, HEADS, KVL), jnp.float32), -6.0, 6.0)
    return queries.astype(jnp.bfloat16)


def strengthened(drawn, own_key, source, target, blocks, factor):
    owner, partner = [(jnp.arange(drawn.shape[axis_at]) // (drawn.shape[axis_at] // blocks)).reshape([-1 if axis == axis_at else 1 for axis in range(drawn.ndim)]) for axis_at in (source, target)]
    chosen = jax.random.permutation(own_key, blocks)[partner]
    strong = (owner == chosen) | (owner == (partner + blocks // 2) % blocks)
    return jnp.where(strong, factor * drawn, drawn)


def block_levels(rng, shape, shards, smallest, high):
    factor_of, own = 1.0, jax.random.fold_in(rng, 6)
    for dim, blocks in shards:
        steps = jnp.exp(jax.random.uniform(jax.random.fold_in(own, dim), (blocks,), jnp.float32, smallest / len(shards), high / len(shards)))
        factor_of = factor_of * jnp.repeat(steps, shape[dim] // blocks).reshape([-1 if axis == dim else 1 for axis in range(len(shape))])
    return factor_of


def scatter_about(stream_key, shape, width, limit, split=(), kind=jnp.bfloat16):
    level = block_levels(stream_key, shape, split, -0.22, 0.18) if split else 1.0
    values = jax.random.normal(stream_key, shape, jnp.float32) * width * level
    return jnp.minimum(jnp.maximum(values, -limit), limit).astype(kind)


def bell_draw_with(key, shape, spread, most, split, heavy, kind=jnp.bfloat16):
    drawn = spread * jax.random.normal(key, shape, jnp.float32)
    if split:
        drawn = drawn * block_levels(key, shape, split, -0.22, 0.18)
    return jnp.clip(strengthened(drawn, jax.random.fold_in(key, 3), *heavy), -most, most).astype(kind)


def setup_inputs(seed: int = 0) -> dict:
    splits = jax.random.split(jax.random.key(seed), 10)
    return {
        "layer_input": bell_draw_with(splits[0], (N_DP, SEQ, D), 1.0, 6.0, ((1, 32), (2, 8)), (1, 2, 32, 2.75)),
        "kv_latent": draw_kv_latent(jax.random.fold_in(splits[9], 71), 0),
        "key_rope": scatter_about(splits[2], (N_DP, SEQ, ROPE), 1.0, 6.0, ((0, 8), (1, 32))),
        "q_latent": draw_q_latent(jax.random.fold_in(splits[9], 71), 0),
        "q_rope": scatter_about(splits[4], (N_DP, SEQ, HEADS, ROPE), 0.5, 3.0, ((0, 8), (1, 32))),
        "saved_output": scatter_about(splits[5], (N_DP, SEQ, HEADS, KVL), 0.5, 4.0, ((0, 8), (1, 32))),
        "w_uv": scatter_about(splits[6], (KVL, HEADS * VHEAD), KVL ** -0.5, 0.25),
        "d_out": scatter_about(splits[7], (N_DP, SEQ, HEADS * VHEAD), 1.0, 6.0, ((0, 8), (1, 32))),
        "blocks": jax.random.permutation(splits[8], 2 * N_CTX).astype(jnp.int32),
    }


softmax_scale = 1.0 / math.sqrt(192.0)

def group_grads(carry, group, latent_keys, rope_keys, positions, value_weight):
    term_lat, term_rope, value_total = carry
    query_lat, query_rope, saved_rows, grad_out, query_pos = group
    wide = jnp.float32
    keys_wide = latent_keys.astype(wide)
    rope_wide = rope_keys.astype(wide)
    scores = jnp.einsum('thk,jk->thj', query_lat.astype(wide), keys_wide)
    scores = scores + jnp.einsum('thr,jr->thj', query_rope.astype(wide), rope_wide)
    scores = scores * softmax_scale
    visible = positions[None, None, :] <= query_pos[:, None, None]
    masked = jnp.where(visible, scores, -jnp.inf)
    row_max = lax.optimization_barrier(jnp.max(masked, axis=2, keepdims=True))
    log_total = row_max + jnp.log(lax.optimization_barrier(jnp.sum(jnp.exp(masked - row_max), axis=2, keepdims=True)))
    probs = jnp.exp(masked - log_total)
    probs_low = probs.astype(jnp.bfloat16)
    grad_lat = jnp.einsum('thv,khv->thk', grad_out.astype(wide), value_weight.astype(wide)).astype(jnp.bfloat16)
    delta = lax.optimization_barrier(jnp.sum(grad_lat.astype(wide) * saved_rows.astype(wide), axis=2, keepdims=True))
    grad_prob = jnp.einsum('thk,jk->thj', grad_lat.astype(wide), keys_wide)
    grad_score = (probs * (grad_prob - delta)).astype(jnp.bfloat16)
    score_wide = grad_score.astype(wide)
    dq_lat = (softmax_scale * jnp.einsum('thj,jk->thk', score_wide, keys_wide)).astype(jnp.bfloat16)
    dq_rope = (softmax_scale * jnp.einsum('thj,jr->thr', score_wide, rope_wide)).astype(jnp.bfloat16)
    part_lat = jnp.einsum('thj,thk->jk', probs_low.astype(wide), grad_lat.astype(wide))
    part_lat = part_lat + softmax_scale * jnp.einsum('thj,thk->jk', score_wide, query_lat.astype(wide))
    part_rope = softmax_scale * jnp.einsum('thj,thr->jr', score_wide, query_rope.astype(wide))
    term_lat = term_lat + lax.optimization_barrier(part_lat.astype(jnp.bfloat16)).astype(wide)
    term_rope = term_rope + lax.optimization_barrier(part_rope.astype(jnp.bfloat16)).astype(wide)
    value_total = value_total + jnp.einsum('thk,thv->khv', saved_rows.astype(wide), grad_out.astype(wide))
    return ((term_lat, term_rope, value_total), (dq_lat, dq_rope))

def reference(layer_input, kv_latent, key_rope, q_latent, q_rope, saved_output, w_uv, d_out, blocks):
    half_rows = TOK_DEV // 2
    row_ids = jnp.arange(SEQ, dtype=jnp.int32)
    positions = (blocks[row_ids // half_rows] * half_rows + row_ids % half_rows).astype(jnp.int32)
    value_weight = w_uv.reshape(KVL, HEADS, VHEAD)
    query_pos = positions.reshape(N_CTX, TOK_DEV)
    value_total = jnp.zeros((KVL, HEADS, VHEAD), jnp.float32)
    down_total = jnp.zeros((D, KVL + ROPE), jnp.float32)
    dql_list, dqr_list, dkv_list, dkr_list = ([], [], [], [])
    for seq_index in range(N_DP):
        groups = (q_latent[seq_index].reshape(N_CTX, TOK_DEV, HEADS, KVL), q_rope[seq_index].reshape(N_CTX, TOK_DEV, HEADS, ROPE), saved_output[seq_index].reshape(N_CTX, TOK_DEV, HEADS, KVL), d_out[seq_index].reshape(N_CTX, TOK_DEV, HEADS, VHEAD), query_pos)
        step_fn = functools.partial(group_grads, latent_keys=kv_latent[seq_index], rope_keys=key_rope[seq_index], positions=positions, value_weight=value_weight)
        start = (jnp.zeros((SEQ, KVL), jnp.float32), jnp.zeros((SEQ, ROPE), jnp.float32), value_total)
        (term_lat, term_rope, value_total), (dq_lat, dq_rope) = lax.scan(step_fn, start, groups)
        dkv_low = term_lat.astype(jnp.bfloat16)
        dkr_low = term_rope.astype(jnp.bfloat16)
        joined = jnp.concatenate([dkv_low, dkr_low], axis=1)
        down_total = down_total + jnp.dot(layer_input[seq_index].T, joined, preferred_element_type=jnp.float32)
        dql_list.append(dq_lat.reshape(SEQ, HEADS, KVL))
        dqr_list.append(dq_rope.reshape(SEQ, HEADS, ROPE))
        dkv_list.append(dkv_low)
        dkr_list.append(dkr_low)
    return (jnp.stack(dql_list), jnp.stack(dqr_list), jnp.stack(dkv_list), jnp.stack(dkr_list), down_total, value_total.reshape(KVL, HEADS * VHEAD))
```

```python
import math

import jax
import jax.numpy as jnp
from jax import lax
from jax.experimental import pallas as pl
from jax.experimental.pallas import tpu as pltpu
from jax.sharding import Mesh, PartitionSpec as P

softmax_scale = 1.0 / math.sqrt(192.0)
log2e = 1.0 / math.log(2.0)
TILE = 256


def nt(a, b):
    return lax.dot_general(a, b, (((1,), (1,)), ((), ())), preferred_element_type=jnp.float32)


def nn(a, b):
    return lax.dot_general(a, b, (((1,), (0,)), ((), ())), preferred_element_type=jnp.float32)


def tn(a, b):
    return lax.dot_general(a, b, (((0,), (0,)), ((), ())), preferred_element_type=jnp.float32)


def attention_grads(own, slots, pieces, queries, query_rope, grads, delta):
    owners, half, packed = pieces[0].shape
    rows, latent = queries.shape
    rope = query_rope.shape[1]
    wide = -(-(latent + rope) // 128) * 128
    pad = wide - latent - rope
    n = len(pieces)
    count = 2 * owners * n
    seq = count * half
    tile = min(TILE, seq)
    per = tile // half
    group = rows // 2
    heads = group // half
    f32, bf16 = jnp.float32, jnp.bfloat16

    def kernel(own_ref, slots_ref, *refs):
        piece_refs, refs = refs[:n], refs[n:]
        q_ref, qr_ref, g_ref, delta_ref, dq_ref, dqr_ref = refs[:6]
        dk_refs, (sorted_keys, wide_q, scores, dq_acc, dk_acc) = refs[6:8], refs[8:]
        zero_pad = jnp.zeros((half, pad), bf16)

        def places():
            for i in range(n):
                for j in range(owners):
                    for side in range(2):
                        slot = slots_ref[(i * owners + j) * 2 + side]
                        yield i, j, side, pl.multiple_of(slot * half, half)

        for i, j, side, start in places():
            sorted_keys[pl.ds(start, half), :latent] = piece_refs[i][
                j, :, side * latent : (side + 1) * latent
            ]
            at = 2 * latent + side * rope
            sorted_keys[pl.ds(start, half), latent:] = jnp.concatenate(
                [piece_refs[i][j, :, at : at + rope], zero_pad], axis=1
            )

        def clear(pos, carry):
            dk_acc[pl.ds(pl.multiple_of(pos * half, half), half), :] = jnp.zeros((half, wide), f32)
            return carry

        lax.fori_loop(0, count, clear, 0)
        wide_q[:, :latent] = q_ref[...]
        wide_q[:, latent:] = jnp.concatenate([qr_ref[...], jnp.zeros((rows, pad), bf16)], axis=1)

        def block_step(which, carry):
            block = own_ref[which]
            base = pl.multiple_of(which * group, group)
            last = block // per
            dq_acc[...] = jnp.zeros((wide, group), f32)
            query_pos = block * half + lax.broadcasted_iota(jnp.int32, (tile, group), 1) // heads

            def score_tile(t):
                start = pl.multiple_of(t * tile, tile)
                s = nt(sorted_keys[pl.ds(start, tile), :], wide_q[pl.ds(base, group), :])
                return s * (softmax_scale * log2e)

            def fold(t, s, m, l):
                start = pl.multiple_of(t * tile, tile)
                scores[pl.ds(start, tile), :] = s
                new = jnp.maximum(m, jnp.max(s, axis=0, keepdims=True))
                l = l * jnp.exp2(m - new) + jnp.sum(jnp.exp2(s - new), axis=0, keepdims=True)
                return new, l

            def score_step(t, carry):
                return fold(t, score_tile(t), *carry)

            first = (jnp.full((1, group), -jnp.inf, f32), jnp.zeros((1, group), f32))
            m, l = lax.fori_loop(0, last, score_step, first)
            key_pos = last * tile + lax.broadcasted_iota(jnp.int32, (tile, group), 0)
            s = jnp.where(key_pos <= query_pos, score_tile(last), -jnp.inf)
            m, l = fold(last, s, m, l)
            log_total = m + jnp.log2(l)
            row_delta = delta_ref[which]

            def grad_step(t, carry):
                start = pl.multiple_of(t * tile, tile)
                g = g_ref[pl.ds(base, group), :]
                p = jnp.exp2(scores[pl.ds(start, tile), :] - log_total)
                dp = nt(sorted_keys[pl.ds(start, tile), :latent], g)
                ds = (p * (softmax_scale * (dp - row_delta))).astype(bf16)
                dk = nn(ds, wide_q[pl.ds(base, group), :])
                dk_acc[pl.ds(start, tile), :latent] += dk[:, :latent] + nn(p.astype(bf16), g)
                dk_acc[pl.ds(start, tile), latent:] += dk[:, latent:]
                dq_acc[...] += tn(sorted_keys[pl.ds(start, tile), :], ds)
                return carry

            lax.fori_loop(0, last + 1, grad_step, 0)
            dq = dq_acc[...].T.astype(bf16)
            dq_ref[pl.ds(base, group), :] = dq[:, :latent]
            dqr_ref[pl.ds(base, group), :] = dq[:, latent : latent + rope]
            return carry

        lax.fori_loop(0, 2, block_step, 0)

        for i, j, side, start in places():
            part = dk_acc[pl.ds(start, half), :].astype(bf16)
            out = dk_refs[i // (n // 2)]
            k = i % (n // 2)
            out[k, j, :, side * latent : (side + 1) * latent] = part[:, :latent]
            at = 2 * latent + side * rope
            out[k, j, :, at : at + rope] = part[:, latent : latent + rope]

    vmem = pl.BlockSpec(memory_space=pltpu.VMEM)
    smem = pl.BlockSpec(memory_space=pltpu.SMEM)
    dk_shape = jax.ShapeDtypeStruct((n // 2, owners, half, packed), bf16)
    return pl.pallas_call(
        kernel,
        out_shape=(
            jax.ShapeDtypeStruct((rows, latent), bf16),
            jax.ShapeDtypeStruct((rows, rope), bf16),
            dk_shape,
            dk_shape,
        ),
        in_specs=[smem, smem] + [vmem] * (n + 4),
        out_specs=(vmem,) * 4,
        scratch_shapes=[
            pltpu.VMEM((seq, wide), bf16),
            pltpu.VMEM((rows, wide), bf16),
            pltpu.VMEM((seq, group), f32),
            pltpu.VMEM((wide, group), f32),
            pltpu.VMEM((seq, wide), f32),
        ],
        compiler_params=pltpu.CompilerParams(vmem_limit_bytes=60 * 1024 * 1024),
        cost_estimate=pl.CostEstimate(
            flops=20 * rows * seq * latent,
            bytes_accessed=20 * 1024 * 1024,
            transcendentals=2 * rows * seq,
        ),
        name="attention_grads",
    )(own, slots, *pieces, queries, query_rope, grads, delta)


def swapped(x, axis):
    return lax.ppermute(x, axis, [(0, 1), (1, 0)])


def shifted(x, axis, by):
    n = lax.axis_size(axis)
    return lax.ppermute(x, axis, [(i, (i + by) % n) for i in range(n)])


def around(x, axis):
    n = lax.axis_size(axis)
    got = [x] * n
    ahead = behind = x
    for k in range(1, n // 2 + 1):
        behind = shifted(behind, axis, 1)
        got[n - k] = behind
        if k < n - n // 2:
            ahead = shifted(ahead, axis, -1)
            got[k] = ahead
    return got


def added(a, b):
    return (a.astype(jnp.float32) + b.astype(jnp.float32)).astype(a.dtype)


def ring_sum(parts, axis):
    n = lax.axis_size(axis)
    up = parts[n // 2]
    for k in range(n // 2 - 1, 0, -1):
        up = added(parts[k], shifted(up, axis, 1))
    up = shifted(up, axis, 1)
    down = parts[n // 2 + 1]
    for k in range(n // 2 + 2, n):
        down = added(parts[k], shifted(down, axis, -1))
    down = shifted(down, axis, -1)
    f32 = jnp.float32
    return parts[0].astype(f32) + up.astype(f32) + down.astype(f32)


def down_part(order, pieces, layer_input):
    count, tokens, width = layer_input.shape
    pairs, half, packed = pieces[0].shape
    cols = packed // 2
    wide = -(-cols // 128) * 128
    latent = (wide - 128) if wide > cols else cols
    rope = cols - latent
    n = len(pieces)

    def kernel(order_ref, *refs):
        piece_refs, (x_ref, out_ref, joined) = refs[:n], refs[n:]
        zero_pad = jnp.zeros((half, wide - cols), jnp.bfloat16)
        for i in range(n):
            for j in range(pairs):
                for side in range(2):
                    row = order_ref[i * pairs + j] * tokens + side * half
                    at = pl.ds(pl.multiple_of(row, half), half)
                    joined[at, :latent] = piece_refs[i][j, :, side * latent : (side + 1) * latent]
                    first = 2 * latent + side * rope
                    joined[at, latent:] = jnp.concatenate(
                        [piece_refs[i][j, :, first : first + rope], zero_pad], axis=1
                    )
        x = x_ref[...].reshape(count * tokens, width)
        out_ref[...] = tn(x, joined[...])[:, :cols].astype(jnp.bfloat16)

    vmem = pl.BlockSpec(memory_space=pltpu.VMEM)
    smem = pl.BlockSpec(memory_space=pltpu.SMEM)
    return pl.pallas_call(
        kernel,
        out_shape=jax.ShapeDtypeStruct((width, cols), jnp.bfloat16),
        in_specs=[smem] + [vmem] * (n + 1),
        out_specs=vmem,
        scratch_shapes=[pltpu.VMEM((count * tokens, wide), jnp.bfloat16)],
        compiler_params=pltpu.CompilerParams(vmem_limit_bytes=40 * 1024 * 1024),
        name="down_part",
    )(order, *pieces, layer_input)


def packed_rows(lat, rope, half):
    return jnp.concatenate([lat[:half], lat[half:], rope[:half], rope[half:]], axis=1)


def body(layer_input, kv_latent, key_rope, q_latent, q_rope, saved_output, w_uv, d_out, blocks):
    wide, bf16 = jnp.float32, jnp.bfloat16
    tokens, latent = kv_latent.shape[1:]
    rope = key_rope.shape[2]
    half = tokens // 2
    heads = q_latent.shape[2]
    rows = tokens * heads
    value_width = w_uv.shape[1] // heads
    n_z, n_y, n_core = (lax.axis_size(a) for a in ("z", "ylo", "core"))
    my_z, my_y, my_core = (lax.axis_index(a) for a in ("z", "ylo", "core"))

    mine = packed_rows(kv_latent[0], key_rope[0], half)
    pair = jnp.stack([mine, swapped(mine, "ylo")])
    near = around(pair, "z")
    pieces = near + [swapped(p, "core") for p in near]
    at_z = (my_z + jnp.arange(n_z, dtype=jnp.int32)) % n_z
    at_y = my_y ^ jnp.arange(n_y, dtype=jnp.int32)
    at_core = my_core ^ jnp.arange(n_core, dtype=jnp.int32)
    owner = (at_z[None, :, None] * n_y + at_y[None, None, :]) * n_core + at_core[:, None, None]
    slots = blocks.reshape(-1, 2)[owner.reshape(-1)].reshape(-1)
    device = (my_z * n_y + my_y) * n_core + my_core
    own = lax.dynamic_slice_in_dim(blocks, 2 * device, 2, 0)

    value_weight = w_uv.reshape(latent, heads, value_width)
    grad_out = d_out[0].reshape(tokens, heads, value_width)
    outputs = saved_output[0]
    grad_lat = jnp.einsum(
        "thv,khv->thk", grad_out, value_weight, preferred_element_type=wide
    ).astype(bf16)
    delta = jnp.sum(grad_lat.astype(wide) * outputs.astype(wide), axis=2)
    value_part = jnp.einsum("thk,thv->khv", outputs, grad_out, preferred_element_type=wide)
    n_dp, n_ctx = lax.axis_size(DP), lax.axis_size(CTX)
    value_part = value_part.astype(bf16).reshape(n_dp, n_ctx, -1, heads * value_width)
    value_part = lax.all_to_all(value_part.swapaxes(0, 1), CTX, 0, 0, tiled=True)

    d_q, d_qr, dk_own, dk_other = attention_grads(
        own,
        slots,
        pieces,
        q_latent.reshape(rows, latent),
        q_rope.reshape(rows, rope),
        grad_lat.reshape(rows, latent),
        delta.reshape(2, 1, rows // 2),
    )
    other = swapped(dk_other, "core")
    summed = ring_sum([added(dk_own[k], other[k]) for k in range(n_z)], "z").astype(bf16)
    summed = added(summed[0], swapped(summed[1], "ylo"))
    d_lat = jnp.concatenate([summed[:, :latent], summed[:, latent : 2 * latent]], axis=0)[None]
    d_rope = jnp.concatenate(
        [summed[:, 2 * latent : 2 * latent + rope], summed[:, 2 * latent + rope :]], axis=0
    )[None]

    dp_pair = jnp.stack([summed, swapped(summed, "yhi")])
    dp_pieces = around(dp_pair, "x")
    n_x = lax.axis_size("x")
    at_x = (lax.axis_index("x") + jnp.arange(n_x, dtype=jnp.int32)) % n_x
    at_hi = lax.axis_index("yhi") ^ jnp.arange(2, dtype=jnp.int32)
    order = (at_hi[None, :] * n_x + at_x[:, None]).reshape(-1)
    part = down_part(order, dp_pieces, layer_input)
    part = part.reshape(n_ctx, -1, latent + rope)
    arrived = lax.all_to_all(part, CTX, 0, 0, tiled=True)
    grad_down = arrived.astype(wide).sum(axis=0)

    value_part = value_part.astype(wide).sum(axis=0).astype(bf16)
    grad_uv = lax.all_to_all(value_part, DP, 0, 0, tiled=True).astype(wide).sum(axis=0)
    return (
        d_q.reshape(q_latent.shape),
        d_qr.reshape(q_rope.shape),
        d_lat,
        d_rope,
        grad_down,
        grad_uv,
    )


DP = ("yhi", "x")
CTX = ("z", "ylo", "core")


def solution(mesh):
    n_dp, n_ctx = mesh.shape["dp"], mesh.shape["ctx"]
    fine = Mesh(mesh.devices.reshape(2, n_dp // 2, n_ctx // 4, 2, 2), DP + CTX)
    in_specs = (
        P(None, CTX, DP),
        P(DP, CTX, None),
        P(DP, CTX, None),
        P(DP, CTX, None, None),
        P(DP, CTX, None, None),
        P(DP, CTX, None, None),
        P(),
        P(DP, CTX, None),
        P(),
    )
    out_specs = (
        P(DP, CTX, None, None),
        P(DP, CTX, None, None),
        P(DP, CTX, None),
        P(DP, CTX, None),
        P(DP + CTX, None),
        P(DP + CTX, None),
    )
    return jax.shard_map(body, mesh=fine, in_specs=in_specs, out_specs=out_specs, check_vma=False)
```

```python
import math

import jax
import jax.numpy as jnp
from jax import lax
from jax.experimental import pallas as pl
from jax.experimental.pallas import tpu as pltpu
from jax.sharding import Mesh, PartitionSpec as P

softmax_scale = 1.0 / math.sqrt(192.0)
log2e = 1.0 / math.log(2.0)
TILE = 256
SPAN = 2
N_DP = 8
N_CTX = 32


def nt(a, b):
    return lax.dot_general(a, b, (((1,), (1,)), ((), ())), preferred_element_type=jnp.float32)


def nn(a, b):
    return lax.dot_general(a, b, (((1,), (0,)), ((), ())), preferred_element_type=jnp.float32)


def tn(a, b):
    return lax.dot_general(a, b, (((0,), (0,)), ((), ())), preferred_element_type=jnp.float32)


def swapped(x, axis):
    return lax.ppermute(x, axis, [(0, 1), (1, 0)])


def shifted(x, axis, by):
    n = lax.axis_size(axis)
    return lax.ppermute(x, axis, [(i, (i + by) % n) for i in range(n)])


def around(x, axis):
    n = lax.axis_size(axis)
    got = [x] * n
    ahead = behind = x
    for k in range(1, n // 2 + 1):
        behind = shifted(behind, axis, 1)
        got[n - k] = behind
        if k < n - n // 2:
            ahead = shifted(ahead, axis, -1)
            got[k] = ahead
    return got


def added(a, b):
    return (a.astype(jnp.float32) + b.astype(jnp.float32)).astype(a.dtype)


def ring_sum(parts, axis):
    n = lax.axis_size(axis)
    up = parts[n // 2]
    for k in range(n // 2 - 1, 0, -1):
        up = added(parts[k], shifted(up, axis, 1))
    up = shifted(up, axis, 1)
    down = parts[n // 2 + 1]
    for k in range(n // 2 + 2, n):
        down = added(parts[k], shifted(down, axis, -1))
    down = shifted(down, axis, -1)
    f32 = jnp.float32
    return parts[0].astype(f32) + up.astype(f32) + down.astype(f32)


def owner_at(me, core, ahead, y):
    n_z, my_z, my_y, my_core = me[0], me[1], me[2], me[3]
    return (lax.rem(my_z + ahead, n_z) * 2 + (my_y ^ y)) * 2 + (my_core ^ core)


def ranks_of(places):
    return [sum((p < q).astype(jnp.int32) for p in places) for q in places]


def seen_blocks(places, block):
    return sum((p <= block).astype(jnp.int32) for p in places)


def key_blocks(me, blocks_ref, aheads, piece_refs):
    found = []
    n = len(aheads)
    for core in range(2):
        for k, ahead in enumerate(aheads):
            for y in range(2):
                owner = owner_at(me, core, ahead, y)
                ref, j = (piece_refs[k], y) if core == 0 else (piece_refs[n + k // 2], k % 2 * 2 + y)
                for side in range(2):
                    found.append((blocks_ref[2 * owner + side], ref, j, side))
    return found


def sort_keys(found, keys_ref, latent, rope, order):
    half, wide = found[0][1].shape[1], keys_ref.shape[1]
    zero_pad = jnp.zeros((half, wide - latent - rope), keys_ref.dtype)
    rows = []
    for (place, ref, j, side), rank in zip(found, ranks_of([f[0] for f in found])):
        order[rank] = place
        at = pl.ds(pl.multiple_of(rank * half, half), half)
        keys_ref[at, :latent] = ref[j, :, side * latent : (side + 1) * latent]
        start = 2 * latent + side * rope
        keys_ref[at, latent:] = jnp.concatenate([ref[j, :, start : start + rope], zero_pad], axis=1)
        rows.append(at)
    return rows


def tile_scores(t, keys, queries, order, block, heads, half):
    per = keys.shape[0] // half
    group = queries.shape[0]
    ahead = block * half + lax.broadcasted_iota(jnp.int32, (1, group), 1) // heads
    row = lax.broadcasted_iota(jnp.int32, (half, group), 0)
    s = nt(keys, queries) * (softmax_scale * log2e)
    return jnp.concatenate(
        [
            jnp.where(
                row <= ahead - order[t * per + k] * half, s[k * half : (k + 1) * half], -jnp.inf
            )
            for k in range(per)
        ],
        axis=0,
    )


vmem = pl.BlockSpec(memory_space=pltpu.VMEM)
smem = pl.BlockSpec(memory_space=pltpu.SMEM)


def call(kernel, name, out_shape, n_smem, operands, scratch, flops, limit=60):
    return pl.pallas_call(
        kernel,
        out_shape=tuple(jax.ShapeDtypeStruct(*o) for o in out_shape),
        in_specs=[smem] * n_smem + [vmem] * (len(operands) - n_smem),
        out_specs=(vmem,) * len(out_shape),
        scratch_shapes=scratch,
        compiler_params=pltpu.CompilerParams(vmem_limit_bytes=limit * 1024 * 1024),
        cost_estimate=pl.CostEstimate(flops=flops, bytes_accessed=4 << 20, transcendentals=0),
        name=name,
    )(*operands)


def pack_keys(lat, rope):
    tokens, latent = lat.shape
    half, width = tokens // 2, rope.shape[1]

    def kernel(lat_ref, rope_ref, out_ref):
        out_ref[:, :latent] = lat_ref[:half]
        out_ref[:, latent : 2 * latent] = lat_ref[half:]
        out_ref[:, 2 * latent :] = jnp.concatenate([rope_ref[:half], rope_ref[half:]], axis=1)

    shape = ((half, 2 * (latent + width)), lat.dtype)
    return call(kernel, "pack_keys", [shape], 0, (lat, rope), [], 1000, 8)[0]


def prepare(me, queries, query_rope, outputs, grad_out, weight):
    rows, latent = queries.shape
    rope = query_rope.shape[1]
    tokens = grad_out.shape[0]
    heads = rows // tokens
    value = grad_out.shape[1] // heads
    wide = latent + 128
    f32, bf16 = jnp.float32, jnp.bfloat16
    n_dp, n_z = N_DP, N_CTX // 4
    each = latent // (n_dp * N_CTX)

    def kernel(me_ref, q_ref, qr_ref, out_ref, d_ref, w_ref, wide_ref, g_ref, delta_ref, v_ref,
               out_wide, g_wide, v_wide):
        wide_ref[:, :latent] = q_ref[...]
        wide_ref[:, latent:] = jnp.concatenate(
            [qr_ref[...], jnp.zeros((rows, wide - latent - rope), bf16)], axis=1
        )
        lanes = [slice(k, k + 128) for k in range(0, latent, 128)]
        for k, lane in enumerate(lanes):
            out_wide[k] = out_ref[:, lane].astype(f32)
        for h in range(heads):
            d = d_ref[:, h * value : (h + 1) * value]
            at = pl.ds(h, tokens, stride=heads)
            g = nt(d, w_ref[:, h * value : (h + 1) * value])
            for k, lane in enumerate(lanes):
                g_wide[k, at, :] = g[:, lane]
                v_wide[pl.ds(h + k * 128 * heads, 128, stride=heads), :] = tn(
                    out_wide[k, at, :].astype(bf16), d
                )
        delta = jnp.zeros((rows, 128), f32)
        for k, lane in enumerate(lanes):
            g = g_wide[k].astype(bf16)
            g_ref[:, lane] = g
            delta += g.astype(f32) * out_wide[k]
        delta = jnp.sum(delta, axis=1, keepdims=True)
        delta = jnp.broadcast_to(delta, (rows, 128)).T[:1]
        delta_ref[0] = delta[:, : rows // 2]
        delta_ref[1] = delta[:, rows // 2 :]
        me = [me_ref[i] for i in range(4)]
        for core in range(2):
            for ahead in range(n_z):
                for y in range(2):
                    owner = owner_at(me, core, ahead, y)
                    slot = (core * n_z + ahead) * 2 + y
                    for r in range(each):
                        parts = []
                        for dp in range(n_dp):
                            row = ((dp * N_CTX + owner) * each + r) * heads
                            parts.append(v_wide[pl.ds(pl.multiple_of(row, heads), heads), :])
                        v_ref[slot, :, r * value : (r + 1) * value] = jnp.concatenate(
                            parts, axis=0
                        ).astype(bf16)

    return call(
        kernel,
        "prepare",
        [
            ((rows, wide), bf16),
            ((rows, latent), bf16),
            ((2, 1, rows // 2), f32),
            ((N_CTX, n_dp * heads, each * value), bf16),
        ],
        1,
        (me, queries, query_rope, outputs, grad_out, weight),
        [
            pltpu.VMEM((latent // 128, rows, 128), f32),
            pltpu.VMEM((latent // 128, rows, 128), f32),
            pltpu.VMEM((latent * heads, value), f32),
        ],
        1000,
    )


def score_step(me, blocks, aheads, pieces, queries, latent, rope, before):
    half = pieces[0].shape[1]
    rows, wide = queries.shape
    keys = 8 * len(aheads) * half
    per, group = TILE // half, rows // 2
    heads = group // half
    f32, bf16 = jnp.float32, jnp.bfloat16
    n = len(pieces)

    def kernel(me_ref, blocks_ref, *refs):
        piece_refs, q_ref, refs = refs[:n], refs[n], refs[n + 1 :]
        if before:
            peak_in, total_in, *refs = refs
        peak_ref, total_ref, keys_ref, order = refs
        me = [me_ref[i] for i in range(4)]
        found = key_blocks(me, blocks_ref, aheads, piece_refs)
        sort_keys(found, keys_ref, latent, rope, order)

        def block_step(which, carry):
            block = blocks_ref[2 * owner_at(me, 0, 0, 0) + which]
            base = pl.multiple_of(which * group, group)

            def tile_step(t, carry):
                m, l = carry
                at = pl.ds(pl.multiple_of(t * TILE, TILE), TILE)
                s = tile_scores(
                    t, keys_ref[at, :], q_ref[pl.ds(base, group), :], order, block, heads, half
                )
                new = jnp.maximum(m, jnp.max(s, axis=0, keepdims=True))
                l = l * jnp.exp2(m - new) + jnp.sum(jnp.exp2(s - new), axis=0, keepdims=True)
                return new, l

            if before:
                begin = (peak_in[which], total_in[which])
            else:
                begin = (jnp.full((1, group), -jnp.inf, f32), jnp.zeros((1, group), f32))
            tiles = (seen_blocks([f[0] for f in found], block) + per - 1) // per
            peak_ref[which], total_ref[which] = lax.fori_loop(0, tiles, tile_step, begin)
            return carry

        lax.fori_loop(0, 2, block_step, 0)

    stat = ((2, 1, group), f32)
    return call(
        kernel,
        "score_step",
        [stat, stat],
        2,
        (me, blocks, *pieces, queries, *before),
        [pltpu.VMEM((keys, wide), bf16), pltpu.SMEM((keys // half,), jnp.int32)],
        rows * keys * wide,
    )


def grad_step(me, blocks, aheads, pieces, queries, grads, delta, stats, values, dq, last):
    half, packed = pieces[0].shape[1:]
    rows, latent = grads.shape
    wide = queries.shape[1]
    cols = packed // 2
    rope = cols - latent
    keys = 8 * len(aheads) * half
    per, group = TILE // half, rows // 2
    heads = group // half
    f32, bf16 = jnp.float32, jnp.bfloat16
    n = len(pieces)
    first = dq is None
    extra = values.shape[2]
    n_z = values.shape[0] // 4

    def kernel(me_ref, blocks_ref, *refs):
        piece_refs, refs = refs[:n], refs[n:]
        q_ref, g_ref, delta_ref, peak_ref, total_ref, v_ref, *refs = refs
        if not first:
            dq_in, *refs = refs
        near_ref, far_ref, *refs = refs
        if last:
            dq_ref, dqr_ref, keys_ref, order, dk_acc, dq_acc = refs
        else:
            dq_acc, keys_ref, order, dk_acc = refs
        me = [me_ref[i] for i in range(4)]
        found = key_blocks(me, blocks_ref, aheads, piece_refs)
        at_rows = sort_keys(found, keys_ref, latent, rope, order)
        dk_acc[...] = jnp.zeros((keys, wide), f32)

        def block_step(which, carry):
            block = blocks_ref[2 * owner_at(me, 0, 0, 0) + which]
            base = pl.multiple_of(which * group, group)
            log_total = peak_ref[which] + jnp.log2(total_ref[which])
            row_delta = delta_ref[which]
            dq_acc[which] = jnp.zeros((wide, group), f32) if first else dq_in[which]

            def tile_step(t, carry):
                at = pl.ds(pl.multiple_of(t * TILE, TILE), TILE)
                q = q_ref[pl.ds(base, group), :]
                g = g_ref[pl.ds(base, group), :]
                s = tile_scores(t, keys_ref[at, :], q, order, block, heads, half)
                p = jnp.exp2(s - log_total)
                dp = nt(keys_ref[at, :latent], g)
                ds = (p * (softmax_scale * (dp - row_delta))).astype(bf16)
                dk = nn(ds, q)
                dk_acc[at, :latent] += dk[:, :latent] + nn(p.astype(bf16), g)
                dk_acc[at, latent:] += dk[:, latent:]
                dq_acc[which] += tn(keys_ref[at, :], ds)
                return carry

            tiles = (seen_blocks([f[0] for f in found], block) + per - 1) // per
            lax.fori_loop(0, tiles, tile_step, 0)
            if last:
                done = dq_acc[which].T.astype(bf16)
                dq_ref[pl.ds(base, group), :] = done[:, :latent]
                dqr_ref[pl.ds(base, group), :] = done[:, latent:cols]
            return carry

        lax.fori_loop(0, 2, block_step, 0)
        for i, at in enumerate(at_rows):
            core, k, y, side = i // (4 * len(aheads)), i // 4 % len(aheads), i // 2 % 2, i % 2
            part = dk_acc[at, :].astype(bf16)
            out = far_ref if core else near_ref
            out[k, y, :, side * latent : (side + 1) * latent] = part[:, :latent]
            start = 2 * latent + side * rope
            out[k, y, :, start : start + rope] = part[:, latent:cols]
            if side == 0:
                out[k, y, :, packed:] = v_ref[(core * n_z + aheads[k]) * 2 + y]

    dk_shape = ((len(aheads), 2, half, packed + extra), bf16)
    dq_shape = (2, wide, group)
    scratch = [
        pltpu.VMEM((keys, wide), bf16),
        pltpu.SMEM((keys // half,), jnp.int32),
        pltpu.VMEM((keys, wide), f32),
    ]
    if last:
        outs = [((rows, latent), bf16), ((rows, rope), bf16)]
        scratch += [pltpu.VMEM(dq_shape, f32)]
    else:
        outs = [(dq_shape, f32)]
    before = () if first else (dq,)
    return call(
        kernel,
        "grad_step",
        [dk_shape, dk_shape] + outs,
        2,
        (me, blocks, *pieces, queries, grads, delta, *stats, values, *before),
        scratch,
        4 * rows * keys * wide,
    )


def down_part(me, pieces, layer_input, latent, rope, heads):
    count, tokens, width = layer_input.shape
    half, packed = pieces[0].shape[1:]
    cols = latent + rope
    wide = latent + 128
    n = len(pieces)
    each = width // N_CTX
    room = -(-each // 16) * 16
    n_z = N_CTX // 4
    f32, bf16 = jnp.float32, jnp.bfloat16
    lanes = packed - 2 * cols

    def kernel(me_ref, *refs):
        piece_refs, refs = refs[:n], refs[n:]
        x_ref, near_ref, far_ref, lat_ref, rope_ref, v_ref, joined, total, v_total = refs
        me = [me_ref[i] for i in range(4)]
        my_x, my_hi = me_ref[4], me_ref[5]
        zero_pad = jnp.zeros((half, wide - cols), bf16)
        values = jnp.zeros((half, lanes), f32)
        for i in range(n):
            for j in range(2):
                dp = (my_hi ^ j) * n + lax.rem(my_x + i, n)
                values += piece_refs[i][j, :, 2 * cols :].astype(f32)
                for side in range(2):
                    at = pl.ds(pl.multiple_of(dp * tokens + side * half, half), half)
                    lat = piece_refs[i][j, :, side * latent : (side + 1) * latent]
                    start = 2 * latent + side * rope
                    rot = piece_refs[i][j, :, start : start + rope]
                    joined[at, :latent] = lat
                    joined[at, latent:] = jnp.concatenate([rot, zero_pad], axis=1)
                    if i == 0 and j == 0:
                        lat_ref[side * half : (side + 1) * half] = lat
                        rope_ref[side * half : (side + 1) * half] = rot
        v_total[...] = values
        mine = v_total[pl.ds(pl.multiple_of((my_hi * n + my_x) * heads, heads), heads), :]
        value = lanes // v_ref.shape[0]
        for r in range(v_ref.shape[0]):
            v_ref[r] = mine[:, r * value : (r + 1) * value]
        total[...] = tn(x_ref[...].reshape(count * tokens, width), joined[...])
        if room > each:
            for ref in (near_ref, far_ref):
                ref[:, each:] = jnp.zeros((N_CTX // 2, room - each, cols), bf16)
        for c in range(N_CTX):
            core, y, z = (c % 2) ^ me[3], (c // 2 % 2) ^ me[2], c // 4
            slot = lax.rem(z - me[1] + n_z, n_z) * 2 + y
            for k, ref in enumerate((near_ref, far_ref)):

                @pl.when(core == k)
                def _():
                    ref[slot, :each] = total[c * each : (c + 1) * each, :cols].astype(bf16)

    shape = ((N_CTX // 2, room, cols), bf16)
    return call(
        kernel,
        "down_part",
        [
            shape,
            shape,
            ((tokens, latent), bf16),
            ((tokens, rope), bf16),
            ((lanes * half // (N_DP * heads * 128), heads, 128), f32),
        ],
        1,
        (me, *pieces, layer_input),
        [
            pltpu.VMEM((count * tokens, wide), bf16),
            pltpu.VMEM((width, wide), f32),
            pltpu.VMEM((half, lanes), f32),
        ],
        1000,
    )


def body(layer_input, kv_latent, key_rope, q_latent, q_rope, saved_output, w_uv, d_out, blocks):
    wide, bf16 = jnp.float32, jnp.bfloat16
    latent, rope = kv_latent.shape[2], key_rope.shape[2]
    heads = q_latent.shape[2]
    n_z = lax.axis_size("z")
    me = jnp.stack(
        [jnp.int32(n_z)] + [lax.axis_index(a) for a in ("z", "ylo", "core", "x", "yhi")]
    )

    mine = pack_keys(kv_latent[0], key_rope[0])
    near = around(jnp.stack([mine, swapped(mine, "ylo")]), "z")
    pairs = [(n_z // 2 - c, (n_z // 2 + 1 + c) % n_z) for c in range(n_z // 2)]
    far = [swapped(jnp.concatenate([near[a], near[b]], axis=0), "core") for a, b in pairs]
    chunks = [range(k, k + SPAN) for k in range(0, n_z // 2, SPAN)]
    aheads = [[a for k in chunk for a in pairs[k]] for chunk in chunks]
    pieces = [
        [near[a] for a in ahead] + [far[k] for k in chunk] for ahead, chunk in zip(aheads, chunks)
    ]

    queries, grads, delta, values = prepare(
        me,
        q_latent.reshape(-1, latent),
        q_rope.reshape(-1, rope),
        saved_output.reshape(-1, latent),
        d_out[0],
        w_uv,
    )
    stats = ()
    for ahead, piece in reversed(list(zip(aheads, pieces))):
        stats = score_step(me, blocks, ahead, piece, queries, latent, rope, stats)
    d_q = up = down = None
    for c, (ahead, piece) in enumerate(zip(aheads, pieces)):
        last = c == len(chunks) - 1
        near_dk, far_dk, *d_q = grad_step(
            me, blocks, ahead, piece, queries, grads, delta, stats, values,
            d_q[0] if d_q else None, last,
        )
        there = swapped(far_dk, "core")
        for k in range(0, len(ahead), 2):
            at_a, at_b = (near_dk[i].astype(wide) + there[i].astype(wide) for i in (k, k + 1))
            if up is not None:
                at_a = at_a + shifted(up, "z", 1).astype(wide)
                at_b = at_b + shifted(down, "z", -1).astype(wide)
            up = at_a.astype(bf16)
            down = at_b if ahead[k + 1] == 0 else at_b.astype(bf16)
    d_q, d_qr = d_q
    summed = down + shifted(up, "z", 1).astype(wide)
    summed = (summed[0] + swapped(summed[1].astype(bf16), "ylo").astype(wide)).astype(bf16)

    dp_pieces = around(jnp.stack([summed, swapped(summed, "yhi")]), "x")
    near_part, far_part, d_lat, d_rope, grad_uv = down_part(
        me, dp_pieces, layer_input, latent, rope, heads
    )
    parts = (near_part.astype(wide) + swapped(far_part, "core").astype(wide)).astype(bf16)
    parts = parts.reshape(n_z, 2, *parts.shape[1:])
    part = ring_sum([parts[k] for k in range(n_z)], "z")
    grad_down = part[0] + swapped(part[1].astype(bf16), "ylo").astype(wide)
    return (
        d_q.reshape(q_latent.shape),
        d_qr.reshape(q_rope.shape),
        d_lat[None],
        d_rope[None],
        grad_down[: layer_input.shape[2] // N_CTX],
        grad_uv.reshape(-1, w_uv.shape[1]),
    )


DP = ("yhi", "x")
CTX = ("z", "ylo", "core")


def solution(mesh):
    n_dp, n_ctx = mesh.shape["dp"], mesh.shape["ctx"]
    fine = Mesh(mesh.devices.reshape(2, n_dp // 2, n_ctx // 4, 2, 2), DP + CTX)
    in_specs = (
        P(None, CTX, DP),
        P(DP, CTX, None),
        P(DP, CTX, None),
        P(DP, CTX, None, None),
        P(DP, CTX, None, None),
        P(DP, CTX, None, None),
        P(),
        P(DP, CTX, None),
        P(),
    )
    out_specs = (
        P(DP, CTX, None, None),
        P(DP, CTX, None, None),
        P(DP, CTX, None),
        P(DP, CTX, None),
        P(DP + CTX, None),
        P(DP + CTX, None),
    )
    return jax.shard_map(body, mesh=fine, in_specs=in_specs, out_specs=out_specs, check_vma=False)
```

```python
import math

import jax
import jax.numpy as jnp
from jax import lax
from jax.experimental import pallas as pl
from jax.experimental.pallas import tpu as pltpu
from jax.sharding import Mesh, PartitionSpec as P


softmax_scale = 1.0 / math.sqrt(192.0)
log2e = 1.0 / math.log(2.0)
TILE = 256
N_DP = 8
N_CTX = 32


def nt(a, b):
    return lax.dot_general(a, b, (((1,), (1,)), ((), ())), preferred_element_type=jnp.float32)


def nn(a, b):
    return lax.dot_general(a, b, (((1,), (0,)), ((), ())), preferred_element_type=jnp.float32)


def tn(a, b):
    return lax.dot_general(a, b, (((0,), (0,)), ((), ())), preferred_element_type=jnp.float32)


def swapped(x, axis):
    return lax.ppermute(x, axis, [(0, 1), (1, 0)])


def shifted(x, axis, by):
    n = lax.axis_size(axis)
    return lax.ppermute(x, axis, [(i, (i + by) % n) for i in range(n)])


def around(x, axis):
    n = lax.axis_size(axis)
    got = [x] * n
    ahead = behind = x
    for k in range(1, n // 2 + 1):
        behind = shifted(behind, axis, 1)
        got[n - k] = behind
        if k < n - n // 2:
            ahead = shifted(ahead, axis, -1)
            got[k] = ahead
    return got


def added(a, b):
    return (a.astype(jnp.float32) + b.astype(jnp.float32)).astype(a.dtype)


def ring_sum(parts, axis):
    n = lax.axis_size(axis)
    up = parts[n // 2]
    for k in range(n // 2 - 1, 0, -1):
        up = added(parts[k], shifted(up, axis, 1))
    up = shifted(up, axis, 1)
    down = parts[n // 2 + 1]
    for k in range(n // 2 + 2, n):
        down = added(parts[k], shifted(down, axis, -1))
    down = shifted(down, axis, -1)
    f32 = jnp.float32
    return parts[0].astype(f32) + up.astype(f32) + down.astype(f32)


def owner_at(me, core, ahead, y):
    n_z, my_z, my_y, my_core = me[0], me[1], me[2], me[3]
    return (lax.rem(my_z + ahead, n_z) * 2 + (my_y ^ y)) * 2 + (my_core ^ core)


def place_keys(me, blocks_ref, aheads, table, order):
    places = []
    for core in range(2):
        for ahead in aheads:
            for y in range(2):
                owner = owner_at(me, core, ahead, y)
                places += [blocks_ref[2 * owner + side] for side in range(2)]
    for i, q in enumerate(places):
        table[i] = q

    def rank_step(i, carry):
        q = table[i]
        rank = sum((p < q).astype(jnp.int32) for p in places)
        table[i] = rank
        order[rank] = q
        return carry

    lax.fori_loop(0, len(places), rank_step, 0)
    return places


def seen_blocks(places, block):
    return sum((p <= block).astype(jnp.int32) for p in places)


def each_block(piece_refs, items, table, half, do):
    n = len(piece_refs) // 2

    def item_step(j, carry):
        for i, ref in enumerate(piece_refs):
            for side in range(2):
                rank = table[(i * items + j) * 2 + side]
                do(i // n, i % n, j, side, pl.ds(pl.multiple_of(rank * half, half), half))
        return carry

    lax.fori_loop(0, items, item_step, 0)


def sort_keys(piece_refs, first, items, table, keys_ref, latent, rope):
    n = len(piece_refs) // 2
    half, wide = piece_refs[0].shape[1], keys_ref.shape[1]
    zero_pad = jnp.zeros((half, wide - latent - rope), keys_ref.dtype)

    def copy(core, i, j, side, at):
        ref = piece_refs[core * n + i]
        j = first + j
        keys_ref[at, :latent] = ref[j, :, side * latent : (side + 1) * latent]
        start = 2 * latent + side * rope
        keys_ref[at, latent:] = jnp.concatenate([ref[j, :, start : start + rope], zero_pad], axis=1)

    each_block(piece_refs, items, table, half, copy)


def tile_scores(t, keys, queries, order, block, heads, half):
    per = keys.shape[0] // half
    group = queries.shape[0]
    ahead = block * half + lax.broadcasted_iota(jnp.int32, (1, group), 1) // heads
    row = lax.broadcasted_iota(jnp.int32, (half, group), 0)
    s = nt(keys, queries) * (softmax_scale * log2e)
    return jnp.concatenate(
        [
            jnp.where(
                row <= ahead - order[t * per + k] * half, s[k * half : (k + 1) * half], -jnp.inf
            )
            for k in range(per)
        ],
        axis=0,
    )


vmem = pl.BlockSpec(memory_space=pltpu.VMEM)
smem = pl.BlockSpec(memory_space=pltpu.SMEM)


def call(kernel, out_shape, n_smem, operands, scratch, flops, limit=60):
    return pl.pallas_call(
        kernel,
        out_shape=tuple(jax.ShapeDtypeStruct(*o) for o in out_shape),
        in_specs=[smem] * n_smem + [vmem] * (len(operands) - n_smem),
        out_specs=(vmem,) * len(out_shape),
        scratch_shapes=scratch,
        compiler_params=pltpu.CompilerParams(vmem_limit_bytes=limit * 1024 * 1024),
        cost_estimate=pl.CostEstimate(flops=flops, bytes_accessed=4 << 20, transcendentals=0),
    )(*operands)


def pack_keys(lat, rope):
    tokens, latent = lat.shape
    half, width = tokens // 2, rope.shape[1]

    def kernel(lat_ref, rope_ref, out_ref):
        out_ref[:, :latent] = lat_ref[:half]
        out_ref[:, latent : 2 * latent] = lat_ref[half:]
        out_ref[:, 2 * latent :] = jnp.concatenate([rope_ref[:half], rope_ref[half:]], axis=1)

    shape = ((half, 2 * (latent + width)), lat.dtype)
    return call(kernel, [shape], 0, (lat, rope), [], 1000, 8)[0]


def prepare(me, queries, query_rope, outputs, grad_out, weight):
    rows, latent = queries.shape
    rope = query_rope.shape[1]
    tokens = grad_out.shape[0]
    heads = rows // tokens
    value = grad_out.shape[1] // heads
    wide = latent + 128
    f32, bf16 = jnp.float32, jnp.bfloat16
    n_dp, n_z = N_DP, N_CTX // 4
    each = latent // (n_dp * N_CTX)

    def kernel(me_ref, q_ref, qr_ref, out_ref, d_ref, w_ref, wide_ref, g_ref, delta_ref, v_ref,
               out_wide, g_wide, v_wide):
        wide_ref[:, :latent] = q_ref[...]
        wide_ref[:, latent:] = jnp.concatenate(
            [qr_ref[...], jnp.zeros((rows, wide - latent - rope), bf16)], axis=1
        )
        lanes = [slice(k, k + 128) for k in range(0, latent, 128)]
        for k, lane in enumerate(lanes):
            out_wide[k] = out_ref[:, lane].astype(f32)

        def head_step(h, carry):
            at = pl.ds(h, tokens, stride=heads)
            column = pl.ds(pl.multiple_of(h * value, value), value)
            d = d_ref[:, column]
            g = nt(d, w_ref[:, column])
            for k, lane in enumerate(lanes):
                g_wide[k, at, :] = g[:, lane]
                v_wide[pl.ds(h + k * 128 * heads, 128, stride=heads), :] = tn(
                    out_wide[k, at, :].astype(bf16), d
                )
            return carry

        lax.fori_loop(0, heads, head_step, 0)
        delta = jnp.zeros((rows, 128), f32)
        for k, lane in enumerate(lanes):
            g = g_wide[k].astype(bf16)
            g_ref[:, lane] = g
            delta += g.astype(f32) * out_wide[k]
        delta = jnp.sum(delta, axis=1, keepdims=True)
        delta = jnp.broadcast_to(delta, (rows, 128)).T[:1]
        delta_ref[0] = delta[:, : rows // 2]
        delta_ref[1] = delta[:, rows // 2 :]
        me = [me_ref[i] for i in range(4)]

        def slot_step(slot, carry):
            owner = owner_at(me, slot // (2 * n_z), slot // 2 % n_z, slot % 2)
            for r in range(each):
                parts = []
                for dp in range(n_dp):
                    row = ((dp * N_CTX + owner) * each + r) * heads
                    parts.append(v_wide[pl.ds(pl.multiple_of(row, heads), heads), :])
                v_ref[slot, :, r * value : (r + 1) * value] = jnp.concatenate(
                    parts, axis=0
                ).astype(bf16)
            return carry

        lax.fori_loop(0, N_CTX, slot_step, 0)

    return call(
        kernel,
        [
            ((rows, wide), bf16),
            ((rows, latent), bf16),
            ((2, 1, rows // 2), f32),
            ((N_CTX, n_dp * heads, each * value), bf16),
        ],
        1,
        (me, queries, query_rope, outputs, grad_out, weight),
        [
            pltpu.VMEM((latent // 128, rows, 128), f32),
            pltpu.VMEM((latent // 128, rows, 128), f32),
            pltpu.VMEM((latent * heads, value), f32),
        ],
        1000,
    )


def score_step(me, blocks, aheads, pieces, queries, latent, rope, before):
    half = pieces[0].shape[1]
    rows, wide = queries.shape
    keys = 8 * len(aheads) * half
    per, group = TILE // half, rows // 2
    heads = group // half
    f32, bf16 = jnp.float32, jnp.bfloat16
    n = len(pieces)

    def kernel(me_ref, blocks_ref, *refs):
        piece_refs, q_ref, refs = refs[:n], refs[n], refs[n + 1 :]
        if before:
            peak_in, total_in, *refs = refs
        peak_ref, total_ref, keys_ref, table, order = refs
        me = [me_ref[i] for i in range(4)]
        places = place_keys(me, blocks_ref, aheads, table, order)
        sort_keys(piece_refs, 0, pieces[0].shape[0], table, keys_ref, latent, rope)

        def block_step(which, carry):
            block = blocks_ref[2 * owner_at(me, 0, 0, 0) + which]
            base = pl.multiple_of(which * group, group)

            def tile_step(t, carry):
                m, l = carry
                at = pl.ds(pl.multiple_of(t * TILE, TILE), TILE)
                s = tile_scores(
                    t, keys_ref[at, :], q_ref[pl.ds(base, group), :], order, block, heads, half
                )
                new = jnp.maximum(m, jnp.max(s, axis=0, keepdims=True))
                l = l * jnp.exp2(m - new) + jnp.sum(jnp.exp2(s - new), axis=0, keepdims=True)
                return new, l

            if before:
                begin = (peak_in[which], total_in[which])
            else:
                begin = (jnp.full((1, group), -jnp.inf, f32), jnp.zeros((1, group), f32))
            tiles = (seen_blocks(places, block) + per - 1) // per
            peak_ref[which], total_ref[which] = lax.fori_loop(0, tiles, tile_step, begin)
            return carry

        lax.fori_loop(0, 2, block_step, 0)

    stat = ((2, 1, group), f32)
    return call(
        kernel,
        [stat, stat],
        2,
        (me, blocks, *pieces, queries, *before),
        [pltpu.VMEM((keys, wide), bf16)] + [pltpu.SMEM((keys // half,), jnp.int32)] * 2,
        rows * keys * wide,
    )


def grad_step(me, blocks, aheads, pieces, queries, grads, delta, stats, values, dq, start, last):
    half, packed = pieces[0].shape[1:]
    rows, latent = grads.shape
    wide = queries.shape[1]
    cols = packed // 2
    rope = cols - latent
    keys = 8 * len(aheads) * half
    per, group = TILE // half, rows // 2
    heads = group // half
    f32, bf16 = jnp.float32, jnp.bfloat16
    n = len(pieces)
    first = dq is None
    extra = values.shape[2]
    n_z = values.shape[0] // 4

    def kernel(me_ref, blocks_ref, *refs):
        piece_refs, refs = refs[:n], refs[n:]
        q_ref, g_ref, delta_ref, peak_ref, total_ref, v_ref, *refs = refs
        if not first:
            dq_in, *refs = refs
        near_ref, far_ref, *refs = refs
        if last:
            dq_ref, dqr_ref, keys_ref, table, order, dk_acc, dq_acc = refs
        else:
            dq_acc, keys_ref, table, order, dk_acc = refs
        me = [me_ref[i] for i in range(4)]
        places = place_keys(me, blocks_ref, aheads, table, order)
        items = 2 * len(aheads)
        sort_keys(piece_refs, start, items, table, keys_ref, latent, rope)

        def clear_step(k, carry):
            at = pl.ds(pl.multiple_of(k * half, half), half)
            dk_acc[at, :] = jnp.zeros((half, wide), f32)
            return carry

        lax.fori_loop(0, keys // half, clear_step, 0)

        def block_step(which, carry):
            block = blocks_ref[2 * owner_at(me, 0, 0, 0) + which]
            base = pl.multiple_of(which * group, group)
            log_total = peak_ref[which] + jnp.log2(total_ref[which])
            row_delta = delta_ref[which]

            def start_step(k, carry):
                at = pl.ds(pl.multiple_of(k * 64, 64), 64)
                dq_acc[which, at] = jnp.zeros((64, group), f32) if first else dq_in[which, at]
                return carry

            lax.fori_loop(0, wide // 64, start_step, 0)

            def tile_step(t, carry):
                at = pl.ds(pl.multiple_of(t * TILE, TILE), TILE)
                q = q_ref[pl.ds(base, group), :]
                g = g_ref[pl.ds(base, group), :]
                s = tile_scores(t, keys_ref[at, :], q, order, block, heads, half)
                p = jnp.exp2(s - log_total)
                dp = nt(keys_ref[at, :latent], g)
                ds = (p * (softmax_scale * (dp - row_delta))).astype(bf16)
                dk = nn(ds, q)
                dk_acc[at, :latent] += dk[:, :latent] + nn(p.astype(bf16), g)
                dk_acc[at, latent:] += dk[:, latent:]
                dq_acc[which] += tn(keys_ref[at, :], ds)
                return carry

            tiles = (seen_blocks(places, block) + per - 1) // per
            lax.fori_loop(0, tiles, tile_step, 0)
            if last:
                done = dq_acc[which].T.astype(bf16)
                dq_ref[pl.ds(base, group), :] = done[:, :latent]
                dqr_ref[pl.ds(base, group), :] = done[:, latent:cols]
            return carry

        lax.fori_loop(0, 2, block_step, 0)

        def unsort(core, i, j, side, at):
            part = dk_acc[at, :].astype(bf16)
            out = far_ref if core else near_ref
            out[j, :, side * latent : (side + 1) * latent] = part[:, :latent]
            at_rope = 2 * latent + side * rope
            out[j, :, at_rope : at_rope + rope] = part[:, latent:cols]

        each_block(piece_refs, items, table, half, unsort)
        for core, out in enumerate((near_ref, far_ref)):
            for k, ahead in enumerate(aheads):
                slot = (core * n_z + ahead) * 2
                out[2 * k : 2 * k + 2, :, packed:] = v_ref[slot : slot + 2]

    dk_shape = ((2 * len(aheads), half, packed + extra), bf16)
    dq_shape = (2, wide, group)
    scratch = [
        pltpu.VMEM((keys, wide), bf16),
        pltpu.SMEM((keys // half,), jnp.int32),
        pltpu.SMEM((keys // half,), jnp.int32),
        pltpu.VMEM((keys, wide), f32),
    ]
    if last:
        outs = [((rows, latent), bf16), ((rows, rope), bf16)]
        scratch += [pltpu.VMEM(dq_shape, f32)]
    else:
        outs = [(dq_shape, f32)]
    before = () if first else (dq,)
    return call(
        kernel,
        [dk_shape, dk_shape] + outs,
        2,
        (me, blocks, *pieces, queries, grads, delta, *stats, values, *before),
        scratch,
        4 * rows * keys * wide,
    )


def down_part(me, pieces, layer_input, latent, rope, heads):
    count, tokens, width = layer_input.shape
    half, packed = pieces[0].shape[1:]
    cols = latent + rope
    wide = latent + 128
    n = len(pieces)
    each = width // N_CTX
    room = -(-each // 16) * 16
    f32, bf16 = jnp.float32, jnp.bfloat16
    lanes = packed - 2 * cols

    def kernel(me_ref, *refs):
        piece_refs, refs = refs[:n], refs[n:]
        x_ref, near_ref, far_ref, lat_ref, rope_ref, v_ref, joined, total, placed, v_total = refs
        me = [me_ref[i] for i in range(4)]
        my_x, my_hi = me_ref[4], me_ref[5]
        zero_pad = jnp.zeros((half, wide - cols), bf16)
        values = jnp.zeros((half, lanes), f32)
        for i in range(n):
            for j in range(2):
                dp = (my_hi ^ j) * n + lax.rem(my_x + i, n)
                values += piece_refs[i][j, :, 2 * cols :].astype(f32)
                for side in range(2):
                    at = pl.ds(pl.multiple_of(dp * tokens + side * half, half), half)
                    lat = piece_refs[i][j, :, side * latent : (side + 1) * latent]
                    start = 2 * latent + side * rope
                    rot = piece_refs[i][j, :, start : start + rope]
                    joined[at, :latent] = lat
                    joined[at, latent:] = jnp.concatenate([rot, zero_pad], axis=1)
                    if i == 0 and j == 0:
                        lat_ref[side * half : (side + 1) * half] = lat
                        rope_ref[side * half : (side + 1) * half] = rot
        v_total[...] = values
        mine = v_total[pl.ds(pl.multiple_of((my_hi * n + my_x) * heads, heads), heads), :]
        value = lanes // v_ref.shape[0]
        for r in range(v_ref.shape[0]):
            v_ref[r] = mine[:, r * value : (r + 1) * value]
        total[...] = tn(x_ref[...].reshape(count * tokens, width), joined[...])
        for c in range(N_CTX):
            placed[c, :each] = total[c * each : (c + 1) * each]
            if room > each:
                placed[c, each:] = jnp.zeros((room - each, wide), f32)

        def slot_step(slot, carry):
            for core, ref in enumerate((near_ref, far_ref)):
                owner = owner_at(me, core, slot // 2, slot % 2)
                ref[slot] = placed[owner, :, :cols].astype(bf16)
            return carry

        lax.fori_loop(0, N_CTX // 2, slot_step, 0)

    shape = ((N_CTX // 2, room, cols), bf16)
    return call(
        kernel,
        [
            shape,
            shape,
            ((tokens, latent), bf16),
            ((tokens, rope), bf16),
            ((lanes * half // (N_DP * heads * 128), heads, 128), f32),
        ],
        1,
        (me, *pieces, layer_input),
        [
            pltpu.VMEM((count * tokens, wide), bf16),
            pltpu.VMEM((width, wide), f32),
            pltpu.VMEM((N_CTX, room, wide), f32),
            pltpu.VMEM((half, lanes), f32),
        ],
        1000,
    )


def body(layer_input, kv_latent, key_rope, q_latent, q_rope, saved_output, w_uv, d_out, blocks):
    wide, bf16 = jnp.float32, jnp.bfloat16
    latent, rope = kv_latent.shape[2], key_rope.shape[2]
    heads = q_latent.shape[2]
    n_z = lax.axis_size("z")
    me = jnp.stack(
        [jnp.int32(n_z)] + [lax.axis_index(a) for a in ("z", "ylo", "core", "x", "yhi")]
    )

    mine = pack_keys(kv_latent[0], key_rope[0])
    near = around(jnp.stack([mine, swapped(mine, "ylo")]), "z")
    pairs = [(n_z // 2 - c, (n_z // 2 + 1 + c) % n_z) for c in range(n_z // 2)]
    last = len(pairs) // 2
    spans = [[k] for k in range(last)] + [range(last, len(pairs))]
    near = [jnp.concatenate([near[a] for k in span for a in pairs[k]], axis=0) for span in spans]
    far = [swapped(x, "core") for x in near]

    queries, grads, delta, values = prepare(
        me,
        q_latent.reshape(-1, latent),
        q_rope.reshape(-1, rope),
        saved_output.reshape(-1, latent),
        d_out[0],
        w_uv,
    )
    stats = ()
    for k in (slice(last, None), slice(0, last)):
        aheads = [a for pair in pairs[k] for a in pair]
        stats = score_step(me, blocks, aheads, near[k] + far[k], queries, latent, rope, stats)
    d_q = up = down = None
    for c, pair in enumerate(pairs):
        k, start = min(c, last), 4 * max(c - last, 0)
        piece = [x[k] for x in (near, far)]
        near_dk, far_dk, *d_q = grad_step(
            me, blocks, pair, piece, queries, grads, delta, stats, values,
            d_q[0] if d_q else None, start, c == len(pairs) - 1,
        )
        there = swapped(far_dk, "core")
        both = near_dk.astype(wide) + there.astype(wide)
        at_a, at_b = both[:2], both[2:]
        if c:
            up = shifted(up, "z", 1)
            at_a = at_a + up.astype(wide)
            at_b = at_b + shifted(down, "z", -1).astype(wide)
        up = at_a.astype(bf16)
        down = at_b if pair[1] == 0 else at_b.astype(bf16)
    d_q, d_qr = d_q
    summed = down + shifted(up, "z", 1).astype(wide)
    summed = (summed[0] + swapped(summed[1].astype(bf16), "ylo").astype(wide)).astype(bf16)

    dp_pieces = around(jnp.stack([summed, swapped(summed, "yhi")]), "x")
    near_part, far_part, d_lat, d_rope, grad_uv = down_part(
        me, dp_pieces, layer_input, latent, rope, heads
    )
    parts = (near_part.astype(wide) + swapped(far_part, "core").astype(wide)).astype(bf16)
    parts = parts.reshape(n_z, 2, *parts.shape[1:])
    part = ring_sum([parts[k] for k in range(n_z)], "z")
    grad_down = part[0] + swapped(part[1].astype(bf16), "ylo").astype(wide)
    return (
        d_q.reshape(q_latent.shape),
        d_qr.reshape(q_rope.shape),
        d_lat[None],
        d_rope[None],
        grad_down[: layer_input.shape[2] // N_CTX],
        grad_uv.reshape(-1, w_uv.shape[1]),
    )


DP = ("yhi", "x")
CTX = ("z", "ylo", "core")


def solution(mesh):
    n_dp, n_ctx = mesh.shape["dp"], mesh.shape["ctx"]
    fine = Mesh(mesh.devices.reshape(2, n_dp // 2, n_ctx // 4, 2, 2), DP + CTX)
    in_specs = (
        P(None, CTX, DP),
        P(DP, CTX, None),
        P(DP, CTX, None),
        P(DP, CTX, None, None),
        P(DP, CTX, None, None),
        P(DP, CTX, None, None),
        P(),
        P(DP, CTX, None),
        P(),
    )
    out_specs = (
        P(DP, CTX, None, None),
        P(DP, CTX, None, None),
        P(DP, CTX, None),
        P(DP, CTX, None),
        P(DP + CTX, None),
        P(DP + CTX, None),
    )

    return jax.shard_map(body, mesh=fine, in_specs=in_specs, out_specs=out_specs, check_vma=False)
```

```python
import math

import jax
import jax.numpy as jnp
from jax import lax
from jax.experimental import pallas as pl
from jax.experimental.pallas import tpu as pltpu
from jax.sharding import Mesh, PartitionSpec as P


softmax_scale = 1.0 / math.sqrt(192.0)
log2e = 1.0 / math.log(2.0)
TILE = 256
N_DP = 8
N_CTX = 32


def nt(a, b):
    return lax.dot_general(a, b, (((1,), (1,)), ((), ())), preferred_element_type=jnp.float32)


def nn(a, b):
    return lax.dot_general(a, b, (((1,), (0,)), ((), ())), preferred_element_type=jnp.float32)


def tn(a, b):
    return lax.dot_general(a, b, (((0,), (0,)), ((), ())), preferred_element_type=jnp.float32)


def swapped(x, axis):
    return lax.ppermute(x, axis, [(0, 1), (1, 0)])


def shifted(x, axis, by):
    n = lax.axis_size(axis)
    return lax.ppermute(x, axis, [(i, (i + by) % n) for i in range(n)])


def added(a, b):
    return (a.astype(jnp.float32) + b.astype(jnp.float32)).astype(a.dtype)


def ring_sum(parts, axis):
    n = lax.axis_size(axis)
    up = parts[n // 2]
    for k in range(n // 2 - 1, 0, -1):
        up = added(parts[k], shifted(up, axis, 1))
    up = shifted(up, axis, 1)
    down = parts[n // 2 + 1]
    for k in range(n // 2 + 2, n):
        down = added(parts[k], shifted(down, axis, -1))
    down = shifted(down, axis, -1)
    f32 = jnp.float32
    return parts[0].astype(f32) + up.astype(f32) + down.astype(f32)


def owner_at(me, core, ahead, y):
    n_z, my_z, my_y, my_core = me[0], me[1], me[2], me[3]
    return (lax.rem(my_z + ahead, n_z) * 2 + (my_y ^ y)) * 2 + (my_core ^ core)


vmem = pl.BlockSpec(memory_space=pltpu.VMEM)
smem = pl.BlockSpec(memory_space=pltpu.SMEM)


def call(kernel, out_shape, n_smem, operands, scratch, flops, limit=60):
    return pl.pallas_call(
        kernel,
        out_shape=tuple(jax.ShapeDtypeStruct(*o) for o in out_shape),
        in_specs=[smem] * n_smem + [vmem] * (len(operands) - n_smem),
        out_specs=(vmem,) * len(out_shape),
        scratch_shapes=scratch,
        compiler_params=pltpu.CompilerParams(vmem_limit_bytes=limit * 1024 * 1024),
        cost_estimate=pl.CostEstimate(flops=flops, bytes_accessed=4 << 20, transcendentals=0),
    )(*operands)


def pack_keys(lat, rope):
    tokens, latent = lat.shape
    half, width = tokens // 2, rope.shape[1]

    def kernel(lat_ref, rope_ref, out_ref):
        out_ref[:, :latent] = lat_ref[:half]
        out_ref[:, latent : 2 * latent] = lat_ref[half:]
        out_ref[:, 2 * latent :] = jnp.concatenate([rope_ref[:half], rope_ref[half:]], axis=1)

    shape = ((half, 2 * (latent + width)), lat.dtype)
    return call(kernel, [shape], 0, (lat, rope), [], 1000, 8)[0]


def prepare(me, queries, query_rope, outputs, grad_out, weight):
    rows, latent = queries.shape
    rope = query_rope.shape[1]
    tokens = grad_out.shape[0]
    heads = rows // tokens
    value = grad_out.shape[1] // heads
    wide = latent + 128
    f32, bf16 = jnp.float32, jnp.bfloat16
    n_dp, n_z = N_DP, N_CTX // 4
    each = latent // (n_dp * N_CTX)

    def kernel(me_ref, q_ref, qr_ref, out_ref, d_ref, w_ref, wide_ref, g_ref, delta_ref, v_ref,
               out_wide, g_wide, v_wide):
        wide_ref[:, :latent] = q_ref[...]
        wide_ref[:, latent:] = jnp.concatenate(
            [qr_ref[...], jnp.zeros((rows, wide - latent - rope), bf16)], axis=1
        )
        lanes = [slice(k, k + 128) for k in range(0, latent, 128)]
        for k, lane in enumerate(lanes):
            out_wide[k] = out_ref[:, lane].astype(f32)

        def head_step(h, carry):
            at = pl.ds(h, tokens, stride=heads)
            column = pl.ds(pl.multiple_of(h * value, value), value)
            d = d_ref[:, column]
            g = nt(d, w_ref[:, column])
            for k, lane in enumerate(lanes):
                g_wide[k, at, :] = g[:, lane]
                v_wide[pl.ds(h + k * 128 * heads, 128, stride=heads), :] = tn(
                    out_wide[k, at, :].astype(bf16), d
                )
            return carry

        lax.fori_loop(0, heads, head_step, 0)
        delta = jnp.zeros((rows, 128), f32)
        for k, lane in enumerate(lanes):
            g = g_wide[k].astype(bf16)
            g_ref[:, lane] = g
            delta += g.astype(f32) * out_wide[k]
        delta = jnp.sum(delta, axis=1, keepdims=True)
        delta = jnp.broadcast_to(delta, (rows, 128)).T[:1]
        delta_ref[0] = delta[:, : rows // 2]
        delta_ref[1] = delta[:, rows // 2 :]
        me = [me_ref[i] for i in range(4)]

        def slot_step(slot, carry):
            owner = owner_at(me, slot // (2 * n_z), slot // 2 % n_z, slot % 2)
            for r in range(each):
                parts = []
                for dp in range(n_dp):
                    row = ((dp * N_CTX + owner) * each + r) * heads
                    parts.append(v_wide[pl.ds(pl.multiple_of(row, heads), heads), :])
                v_ref[slot, :, r * value : (r + 1) * value] = jnp.concatenate(
                    parts, axis=0
                ).astype(bf16)
            return carry

        lax.fori_loop(0, N_CTX, slot_step, 0)

    return call(
        kernel,
        [
            ((rows, wide), bf16),
            ((rows, latent), bf16),
            ((2, 1, rows // 2), f32),
            ((N_CTX, n_dp * heads, each * value), bf16),
        ],
        1,
        (me, queries, query_rope, outputs, grad_out, weight),
        [
            pltpu.VMEM((latent // 128, rows, 128), f32),
            pltpu.VMEM((latent // 128, rows, 128), f32),
            pltpu.VMEM((latent * heads, value), f32),
        ],
        1000,
    )


def attention(me, blocks, pieces, items, queries, grads, delta, values):
    half, packed = pieces[0].shape[1:]
    rows, latent = grads.shape
    wide = queries.shape[1]
    cols = packed // 2
    rope = cols - latent
    count = 2 * N_CTX
    seq = count * half
    per, group = TILE // half, rows // 2
    heads = group // half
    f32, bf16 = jnp.float32, jnp.bfloat16
    n = len(pieces)
    extra = values.shape[2]
    n_z = N_CTX // 4

    def kernel(me_ref, blocks_ref, *refs):
        piece_refs, refs = refs[:n], refs[n:]
        q_ref, g_ref, delta_ref, v_ref, dq_ref, dqr_ref, near_ref, far_ref, *refs = refs
        keys_ref, table, scores, dk_acc, dq_acc = refs
        me = [me_ref[i] for i in range(4)]
        zero_pad = jnp.zeros((half, wide - cols), bf16)
        first = 0
        for ref, places in zip(piece_refs, items):
            for j, place in enumerate(places):
                table[first + j] = owner_at(me, *place)

            def sort_step(j, carry, ref=ref, first=first):
                owner = table[first + j]
                for side in range(2):
                    row = blocks_ref[2 * owner + side] * half
                    at = pl.ds(pl.multiple_of(row, half), half)
                    keys_ref[at, :latent] = ref[j, :, side * latent : (side + 1) * latent]
                    start = 2 * latent + side * rope
                    keys_ref[at, latent:] = jnp.concatenate(
                        [ref[j, :, start : start + rope], zero_pad], axis=1
                    )
                return carry

            lax.fori_loop(0, len(places), sort_step, 0)
            first += len(places)

        device = owner_at(me, 0, 0, 0)
        swap = (blocks_ref[2 * device + 1] > blocks_ref[2 * device]).astype(jnp.int32)
        top = jnp.maximum(blocks_ref[2 * device + 1], blocks_ref[2 * device]) // per

        def block_step(turn, carry):
            which = turn ^ swap
            block = blocks_ref[2 * device + which]
            base = pl.multiple_of(which * group, group)
            final = block // per

            def score_tile(t):
                at = pl.ds(pl.multiple_of(t * TILE, TILE), TILE)
                s = nt(keys_ref[at, :], q_ref[pl.ds(base, group), :])
                return s * (softmax_scale * log2e)

            def fold(t, s, m, l):
                scores[pl.ds(pl.multiple_of(t * TILE, TILE), TILE), :] = s
                new = jnp.maximum(m, jnp.max(s, axis=0, keepdims=True))
                l = l * jnp.exp2(m - new) + jnp.sum(jnp.exp2(s - new), axis=0, keepdims=True)
                return new, l

            begin = (jnp.full((1, group), -jnp.inf, f32), jnp.zeros((1, group), f32))
            m, l = lax.fori_loop(0, final, lambda t, c: fold(t, score_tile(t), *c), begin)
            ahead = block * half + lax.broadcasted_iota(jnp.int32, (1, group), 1) // heads
            row = lax.broadcasted_iota(jnp.int32, (TILE, group), 0)
            s = jnp.where(row <= ahead - final * TILE, score_tile(final), -jnp.inf)
            m, l = fold(final, s, m, l)
            log_total = m + jnp.log2(l)
            row_delta = delta_ref[which]
            dq_acc[...] = jnp.zeros((wide, group), f32)

            def tile_step(t, carry):
                at = pl.ds(pl.multiple_of(t * TILE, TILE), TILE)
                g = g_ref[pl.ds(base, group), :]
                p = jnp.exp2(scores[at, :] - log_total)
                dp = nt(keys_ref[at, :latent], g)
                ds = (p * (softmax_scale * (dp - row_delta))).astype(bf16)
                dk = nn(ds, q_ref[pl.ds(base, group), :])
                before = jnp.where(turn == 0, 0.0, dk_acc[at, :])
                dk_acc[at, :latent] = (
                    before[:, :latent] + dk[:, :latent] + nn(p.astype(bf16), g)
                )
                dk_acc[at, latent:] = before[:, latent:] + dk[:, latent:]
                dq_acc[...] += tn(keys_ref[at, :], ds)
                return carry

            lax.fori_loop(0, final + 1, tile_step, 0)
            done = dq_acc[...].T.astype(bf16)
            dq_ref[pl.ds(base, group), :] = done[:, :latent]
            dqr_ref[pl.ds(base, group), :] = done[:, latent:cols]
            return carry

        lax.fori_loop(0, 2, block_step, 0)

        def unsort_step(j, carry):
            for core, out in enumerate((near_ref, far_ref)):
                owner = owner_at(me, core, j // 2, j % 2)
                for side in range(2):
                    place = blocks_ref[2 * owner + side]
                    at = pl.ds(pl.multiple_of(place * half, half), half)
                    part = jnp.where(place // per <= top, dk_acc[at, :], 0.0).astype(bf16)
                    out[j, :, side * latent : (side + 1) * latent] = part[:, :latent]
                    start = 2 * latent + side * rope
                    out[j, :, start : start + rope] = part[:, latent:cols]
                out[j, :, packed:] = v_ref[core * 2 * n_z + j]
            return carry

        lax.fori_loop(0, 2 * n_z, unsort_step, 0)

    dk_shape = ((2 * n_z, half, packed + extra), bf16)
    return call(
        kernel,
        [((rows, latent), bf16), ((rows, rope), bf16), dk_shape, dk_shape],
        2,
        (me, blocks, *pieces, queries, grads, delta, values),
        [
            pltpu.VMEM((seq, wide), bf16),
            pltpu.SMEM((N_CTX,), jnp.int32),
            pltpu.VMEM((seq, group), f32),
            pltpu.VMEM((seq, wide), f32),
            pltpu.VMEM((wide, group), f32),
        ],
        5 * rows * seq * wide,
    )


def down_part(me, pieces, items, layer_input, latent, rope, heads):
    count, tokens, width = layer_input.shape
    half, packed = pieces[0].shape[1:]
    cols = latent + rope
    wide = latent + 128
    n = len(pieces)
    each = width // N_CTX
    room = -(-each // 16) * 16
    f32, bf16 = jnp.float32, jnp.bfloat16
    lanes = packed - 2 * cols
    n_x = N_DP // 2

    def kernel(me_ref, *refs):
        piece_refs, refs = refs[:n], refs[n:]
        x_ref, near_ref, far_ref, lat_ref, rope_ref, v_ref, joined, total, placed, v_total = refs
        me = [me_ref[i] for i in range(4)]
        my_x, my_hi = me_ref[4], me_ref[5]
        zero_pad = jnp.zeros((half, wide - cols), bf16)
        values = jnp.zeros((half, lanes), f32)
        for i, places in enumerate(items):
            for j, (ahead, hi) in enumerate(places):
                dp = (my_hi ^ hi) * n_x + lax.rem(my_x + ahead, n_x)
                values += piece_refs[i][j, :, 2 * cols :].astype(f32)
                for side in range(2):
                    at = pl.ds(pl.multiple_of(dp * tokens + side * half, half), half)
                    lat = piece_refs[i][j, :, side * latent : (side + 1) * latent]
                    start = 2 * latent + side * rope
                    rot = piece_refs[i][j, :, start : start + rope]
                    joined[at, :latent] = lat
                    joined[at, latent:] = jnp.concatenate([rot, zero_pad], axis=1)
                    if i == 0 and j == 0:
                        lat_ref[side * half : (side + 1) * half] = lat
                        rope_ref[side * half : (side + 1) * half] = rot
        v_total[...] = values
        mine = v_total[pl.ds(pl.multiple_of((my_hi * n_x + my_x) * heads, heads), heads), :]
        value = lanes // v_ref.shape[0]
        for r in range(v_ref.shape[0]):
            v_ref[r] = mine[:, r * value : (r + 1) * value]
        total[...] = tn(x_ref[...].reshape(count * tokens, width), joined[...])
        for c in range(N_CTX):
            placed[c, :each] = total[c * each : (c + 1) * each]
            if room > each:
                placed[c, each:] = jnp.zeros((room - each, wide), f32)

        def slot_step(slot, carry):
            for core, ref in enumerate((near_ref, far_ref)):
                owner = owner_at(me, core, slot // 2, slot % 2)
                ref[slot] = placed[owner, :, :cols].astype(bf16)
            return carry

        lax.fori_loop(0, N_CTX // 2, slot_step, 0)

    shape = ((N_CTX // 2, room, cols), bf16)
    return call(
        kernel,
        [
            shape,
            shape,
            ((tokens, latent), bf16),
            ((tokens, rope), bf16),
            ((lanes * half // (N_DP * heads * 128), heads, 128), f32),
        ],
        1,
        (me, *pieces, layer_input),
        [
            pltpu.VMEM((count * tokens, wide), bf16),
            pltpu.VMEM((width, wide), f32),
            pltpu.VMEM((N_CTX, room, wide), f32),
            pltpu.VMEM((half, lanes), f32),
        ],
        1000,
    )


def body(layer_input, kv_latent, key_rope, q_latent, q_rope, saved_output, w_uv, d_out, blocks):
    wide, bf16 = jnp.float32, jnp.bfloat16
    latent, rope = kv_latent.shape[2], key_rope.shape[2]
    heads = q_latent.shape[2]
    n_z = lax.axis_size("z")
    me = jnp.stack(
        [jnp.int32(n_z)] + [lax.axis_index(a) for a in ("z", "ylo", "core", "x", "yhi")]
    )

    mine = pack_keys(kv_latent[0], key_rope[0])
    ahead, behind = mine, mine
    groups, items, group, places = [], [], [], []
    for k in range(n_z // 2 + 1):
        if k:
            behind = shifted(behind, "z", 1)
            if k < n_z // 2:
                ahead = shifted(ahead, "z", -1)
        at_z = sorted({k, (n_z - k) % n_z})
        here = jnp.stack([ahead, behind][: len(at_z)] if k < n_z // 2 else [behind])
        there = swapped(here, "ylo")
        group += [here, there]
        places += [(z, y) for y in range(2) for z in at_z]
        if k in (n_z // 4, n_z // 2):
            groups.append(jnp.concatenate(group, axis=0))
            items.append(places)
            group, places = [], []
    pieces = groups + [swapped(x, "core") for x in groups]
    items = [[(core, *place) for place in p] for core in range(2) for p in items]

    queries, grads, delta, values = prepare(
        me,
        q_latent.reshape(-1, latent),
        q_rope.reshape(-1, rope),
        saved_output.reshape(-1, latent),
        d_out[0],
        w_uv,
    )
    d_q, d_qr, near_dk, far_dk = attention(
        me, blocks, pieces, items, queries, grads, delta, values
    )
    near_dk = near_dk.reshape(n_z, 2, *near_dk.shape[1:]).astype(wide)
    far_dk = swapped(far_dk, "core").reshape(near_dk.shape).astype(wide)
    summed = ring_sum([(near_dk[k] + far_dk[k]).astype(bf16) for k in range(n_z)], "z")
    summed = summed.astype(bf16)

    flipped = [(i, 3 - i) for i in range(4)]
    summed = jnp.stack(
        [
            added(summed[0], swapped(summed[1], "ylo")),
            added(swapped(summed[0], "yhi"), lax.ppermute(summed[1], ("yhi", "ylo"), flipped)),
        ]
    )

    n_x = lax.axis_size("x")
    after, before = shifted(summed, "x", -1), shifted(summed, "x", 1)
    opposite = [shifted(before[:1], "x", 1), shifted(after[1:], "x", -1)]
    dp_pieces = [summed, after, before] + opposite
    dp_items = [[(k, hi) for hi in range(2)] for k in (0, 1, n_x - 1)] + [[(2, 0)], [(2, 1)]]
    near_part, far_part, d_lat, d_rope, grad_uv = down_part(
        me, dp_pieces, dp_items, layer_input, latent, rope, heads
    )
    parts = (near_part.astype(wide) + swapped(far_part, "core").astype(wide)).astype(bf16)
    parts = parts.reshape(n_z, 2, *parts.shape[1:])
    part = ring_sum([parts[k] for k in range(n_z)], "z")
    grad_down = part[0] + swapped(part[1].astype(bf16), "ylo").astype(wide)
    return (
        d_q.reshape(q_latent.shape),
        d_qr.reshape(q_rope.shape),
        d_lat[None],
        d_rope[None],
        grad_down[: layer_input.shape[2] // N_CTX],
        grad_uv.reshape(-1, w_uv.shape[1]),
    )


DP = ("yhi", "x")
CTX = ("z", "ylo", "core")


def solution(mesh):
    n_dp, n_ctx = mesh.shape["dp"], mesh.shape["ctx"]
    fine = Mesh(mesh.devices.reshape(2, n_dp // 2, n_ctx // 4, 2, 2), DP + CTX)
    in_specs = (
        P(None, CTX, DP),
        P(DP, CTX, None),
        P(DP, CTX, None),
        P(DP, CTX, None, None),
        P(DP, CTX, None, None),
        P(DP, CTX, None, None),
        P(),
        P(DP, CTX, None),
        P(),
    )
    out_specs = (
        P(DP, CTX, None, None),
        P(DP, CTX, None, None),
        P(DP, CTX, None),
        P(DP, CTX, None),
        P(DP + CTX, None),
        P(DP + CTX, None),
    )

    return jax.shard_map(body, mesh=fine, in_specs=in_specs, out_specs=out_specs, check_vma=False)
```

```python
import math

import jax
import jax.numpy as jnp
from jax import lax
from jax.experimental import pallas as pl
from jax.experimental.pallas import tpu as pltpu
from jax.sharding import Mesh, PartitionSpec as P


softmax_scale = 1.0 / math.sqrt(192.0)
log2e = 1.0 / math.log(2.0)
TILE = 256
N_DP = 8
N_CTX = 32


def nt(a, b):
    return lax.dot_general(a, b, (((1,), (1,)), ((), ())), preferred_element_type=jnp.float32)


def nn(a, b):
    return lax.dot_general(a, b, (((1,), (0,)), ((), ())), preferred_element_type=jnp.float32)


def tn(a, b):
    return lax.dot_general(a, b, (((0,), (0,)), ((), ())), preferred_element_type=jnp.float32)


def swapped(x, axis):
    return lax.ppermute(x, axis, [(0, 1), (1, 0)])


def shifted(x, axis, by):
    n = lax.axis_size(axis)
    return lax.ppermute(x, axis, [(i, (i + by) % n) for i in range(n)])


def ring_sum(parts, axis):
    n = lax.axis_size(axis)
    f32, bf16 = jnp.float32, jnp.bfloat16
    up, down = (parts[k].astype(bf16) for k in (n // 2, n // 2 + 1))
    for k in range(n // 2 - 1, -1, -1):
        if k:
            up = (parts[k].astype(f32) + shifted(up, axis, 1).astype(f32)).astype(bf16)
        if 0 < k < n // 2 - 1:
            down = (parts[n - k].astype(f32) + shifted(down, axis, -1).astype(f32)).astype(bf16)
    up, down = shifted(up, axis, 1), shifted(down, axis, -1)
    return parts[0].astype(f32) + up.astype(f32) + down.astype(f32)


def owner_at(me, core, ahead, y):
    n_z, my_z, my_y, my_core = me[0], me[1], me[2], me[3]
    return (lax.rem(my_z + ahead, n_z) * 2 + (my_y ^ y)) * 2 + (my_core ^ core)


def batches():
    n = N_CTX // 4
    far = [[n // 2]] + [[k, n - k] for k in range(n // 2 - 1, 0, -1)]
    return far[:-1] + [far[-1] + [0]]


def fill_owners(table, me):
    places = [(z, y) for batch in batches() for y in range(2) for z in batch]
    for core in range(2):
        for i, place in enumerate(places):
            table[core * len(places) + i] = owner_at(me, core, *place)


vmem = pl.BlockSpec(memory_space=pltpu.VMEM)
smem = pl.BlockSpec(memory_space=pltpu.SMEM)


def call(kernel, out_shape, n_smem, operands, scratch, flops, limit=60):
    return pl.pallas_call(
        kernel,
        out_shape=tuple(jax.ShapeDtypeStruct(*o) for o in out_shape),
        in_specs=[smem] * n_smem + [vmem] * (len(operands) - n_smem),
        out_specs=(vmem,) * len(out_shape),
        scratch_shapes=scratch,
        compiler_params=pltpu.CompilerParams(vmem_limit_bytes=limit * 1024 * 1024),
        cost_estimate=pl.CostEstimate(flops=flops, bytes_accessed=4 << 20, transcendentals=0),
    )(*operands)


def pack_keys(lat, rope):
    tokens, latent = lat.shape
    half, width = tokens // 2, rope.shape[1]

    def kernel(lat_ref, rope_ref, out_ref):
        out_ref[:, :latent] = lat_ref[:half]
        out_ref[:, latent : 2 * latent] = lat_ref[half:]
        out_ref[:, 2 * latent :] = jnp.concatenate([rope_ref[:half], rope_ref[half:]], axis=1)

    shape = ((half, 2 * (latent + width)), lat.dtype)
    return call(kernel, [shape], 0, (lat, rope), [], 1000, 8)[0]


def prepare(queries, query_rope, outputs, grad_out, weight):
    rows, latent = queries.shape
    rope = query_rope.shape[1]
    tokens = grad_out.shape[0]
    heads = rows // tokens
    value = grad_out.shape[1] // heads
    wide = latent + 128
    f32, bf16 = jnp.float32, jnp.bfloat16
    lanes = [slice(k, k + 128) for k in range(0, latent, 128)]

    def kernel(q_ref, qr_ref, out_ref, d_ref, w_ref, wide_ref, g_ref, delta_ref, g_wide):
        wide_ref[:, :latent] = q_ref[...]
        wide_ref[:, latent:] = jnp.concatenate(
            [qr_ref[...], jnp.zeros((rows, wide - latent - rope), bf16)], axis=1
        )

        def head_step(h, carry):
            column = pl.ds(pl.multiple_of(h * value, value), value)
            g = nt(d_ref[:, column], w_ref[:, column])
            for k, lane in enumerate(lanes):
                g_wide[k, pl.ds(h, tokens, stride=heads), :] = g[:, lane]
            return carry

        lax.fori_loop(0, heads, head_step, 0)
        delta = jnp.zeros((rows, 128), f32)
        for k, lane in enumerate(lanes):
            g = g_wide[k].astype(bf16)
            g_ref[:, lane] = g
            delta += g.astype(f32) * out_ref[:, lane].astype(f32)
        delta = jnp.sum(delta, axis=1, keepdims=True)
        delta = jnp.broadcast_to(delta, (rows, 128)).T[:1]
        delta_ref[0] = delta[:, : rows // 2]
        delta_ref[1] = delta[:, rows // 2 :]

    return call(
        kernel,
        [((rows, wide), bf16), ((rows, latent), bf16), ((2, 1, rows // 2), f32)],
        0,
        (queries, query_rope, outputs, grad_out, weight),
        [pltpu.VMEM((latent // 128, rows, 128), f32)],
        1000,
    )


def value_parts(me, outputs, grad_out):
    rows, latent = outputs.shape
    tokens = grad_out.shape[0]
    heads = rows // tokens
    value = grad_out.shape[1] // heads
    f32, bf16 = jnp.float32, jnp.bfloat16
    lanes = [slice(k, k + 128) for k in range(0, latent, 128)]
    n_dp = N_DP
    each = latent // (n_dp * N_CTX)

    def kernel(me_ref, out_ref, d_ref, v_ref, out_wide, v_wide, table):
        fill_owners(table, [me_ref[i] for i in range(4)])
        for k, lane in enumerate(lanes):
            out_wide[k] = out_ref[:, lane].astype(f32)

        def head_step(h, carry):
            d = d_ref[:, pl.ds(pl.multiple_of(h * value, value), value)]
            for k in range(len(lanes)):
                out = out_wide[k, pl.ds(h, tokens, stride=heads), :].astype(bf16)
                v_wide[pl.ds(h + k * 128 * heads, 128, stride=heads), :] = tn(out, d)
            return carry

        lax.fori_loop(0, heads, head_step, 0)

        def slot_step(slot, carry):
            owner = table[slot]
            for r in range(each):
                parts = []
                for dp in range(n_dp):
                    row = ((dp * N_CTX + owner) * each + r) * heads
                    parts.append(v_wide[pl.ds(pl.multiple_of(row, heads), heads), :])
                v_ref[slot, :, r * value : (r + 1) * value] = jnp.concatenate(
                    parts, axis=0
                ).astype(bf16)
            return carry

        lax.fori_loop(0, N_CTX, slot_step, 0)

    return call(
        kernel,
        [((N_CTX, n_dp * heads, each * value), bf16)],
        1,
        (me, outputs, grad_out),
        [
            pltpu.VMEM((latent // 128, rows, 128), f32),
            pltpu.VMEM((latent * heads, value), f32),
            pltpu.SMEM((N_CTX,), jnp.int32),
        ],
        1000,
    )[0]


def attention(me, blocks, pieces, items, queries, grads, delta, values):
    half, packed = pieces[0].shape[1:]
    rows, latent = grads.shape
    wide = queries.shape[1]
    cols = packed // 2
    rope = cols - latent
    count = 2 * N_CTX
    seq = count * half
    per, group = TILE // half, rows // 2
    heads = group // half
    f32, bf16 = jnp.float32, jnp.bfloat16
    n = len(pieces)
    extra = values.shape[2]
    n_z = N_CTX // 4

    def kernel(me_ref, blocks_ref, *refs):
        piece_refs, refs = refs[:n], refs[n:]
        q_ref, g_ref, delta_ref, v_ref, dq_ref, dqr_ref, near_ref, far_ref, *refs = refs
        keys_ref, table, scores, dk_acc, dq_acc = refs
        me = [me_ref[i] for i in range(4)]
        zero_pad = jnp.zeros((half, wide - cols), bf16)
        first = 0
        for ref, places in zip(piece_refs, items):
            for j, place in enumerate(places):
                table[first + j] = owner_at(me, *place)

            def sort_step(j, carry, ref=ref, first=first):
                owner = table[first + j]
                for side in range(2):
                    row = blocks_ref[2 * owner + side] * half
                    at = pl.ds(pl.multiple_of(row, half), half)
                    keys_ref[at, :latent] = ref[j, :, side * latent : (side + 1) * latent]
                    start = 2 * latent + side * rope
                    keys_ref[at, latent:] = jnp.concatenate(
                        [ref[j, :, start : start + rope], zero_pad], axis=1
                    )
                return carry

            lax.fori_loop(0, len(places), sort_step, 0)
            first += len(places)

        device = owner_at(me, 0, 0, 0)
        swap = (blocks_ref[2 * device + 1] > blocks_ref[2 * device]).astype(jnp.int32)
        top = jnp.maximum(blocks_ref[2 * device + 1], blocks_ref[2 * device]) // per

        def block_step(turn, carry):
            which = turn ^ swap
            block = blocks_ref[2 * device + which]
            base = pl.multiple_of(which * group, group)
            final = block // per

            def score_tile(t):
                at = pl.ds(pl.multiple_of(t * TILE, TILE), TILE)
                s = nt(keys_ref[at, :], q_ref[pl.ds(base, group), :])
                return s * (softmax_scale * log2e)

            def fold(t, s, m, l):
                scores[pl.ds(pl.multiple_of(t * TILE, TILE), TILE), :] = s
                new = jnp.maximum(m, jnp.max(s, axis=0, keepdims=True))
                l = l * jnp.exp2(m - new) + jnp.sum(jnp.exp2(s - new), axis=0, keepdims=True)
                return new, l

            begin = (jnp.full((1, group), -jnp.inf, f32), jnp.zeros((1, group), f32))
            m, l = lax.fori_loop(0, final, lambda t, c: fold(t, score_tile(t), *c), begin)
            ahead = block * half + lax.broadcasted_iota(jnp.int32, (1, group), 1) // heads
            row = lax.broadcasted_iota(jnp.int32, (TILE, group), 0)
            s = jnp.where(row <= ahead - final * TILE, score_tile(final), -jnp.inf)
            m, l = fold(final, s, m, l)
            log_total = m + jnp.log2(l)
            row_delta = delta_ref[which]
            dq_acc[...] = jnp.zeros((wide, group), f32)

            def tile_step(t, carry):
                at = pl.ds(pl.multiple_of(t * TILE, TILE), TILE)
                g = g_ref[pl.ds(base, group), :]
                p = jnp.exp2(scores[at, :] - log_total)
                dp = nt(keys_ref[at, :latent], g)
                ds = (p * (softmax_scale * (dp - row_delta))).astype(bf16)
                dk = nn(ds, q_ref[pl.ds(base, group), :])
                before = jnp.where(turn == 0, 0.0, dk_acc[at, :])
                dk_acc[at, :latent] = (
                    before[:, :latent] + dk[:, :latent] + nn(p.astype(bf16), g)
                )
                dk_acc[at, latent:] = before[:, latent:] + dk[:, latent:]
                dq_acc[...] += tn(keys_ref[at, :], ds)
                return carry

            lax.fori_loop(0, final + 1, tile_step, 0)
            done = dq_acc[...].T.astype(bf16)
            dq_ref[pl.ds(base, group), :] = done[:, :latent]
            dqr_ref[pl.ds(base, group), :] = done[:, latent:cols]
            return carry

        lax.fori_loop(0, 2, block_step, 0)
        fill_owners(table, me)

        def unsort_step(j, carry):
            for core, out in enumerate((near_ref, far_ref)):
                owner = table[core * 2 * n_z + j]
                for side in range(2):
                    place = blocks_ref[2 * owner + side]
                    at = pl.ds(pl.multiple_of(place * half, half), half)
                    part = jnp.where(place // per <= top, dk_acc[at, :], 0.0).astype(bf16)
                    out[j, :, side * latent : (side + 1) * latent] = part[:, :latent]
                    start = 2 * latent + side * rope
                    out[j, :, start : start + rope] = part[:, latent:cols]
                out[j, :, packed:] = v_ref[core * 2 * n_z + j]
            return carry

        lax.fori_loop(0, 2 * n_z, unsort_step, 0)

    dk_shape = ((2 * n_z, half, packed + extra), bf16)
    return call(
        kernel,
        [((rows, latent), bf16), ((rows, rope), bf16), dk_shape, dk_shape],
        2,
        (me, blocks, *pieces, queries, grads, delta, values),
        [
            pltpu.VMEM((seq, wide), bf16),
            pltpu.SMEM((N_CTX,), jnp.int32),
            pltpu.VMEM((seq, group), f32),
            pltpu.VMEM((seq, wide), f32),
            pltpu.VMEM((wide, group), f32),
        ],
        5 * rows * seq * wide,
    )


def down_part(me, pieces, items, layer_input, latent, rope, heads):
    count, tokens, width = layer_input.shape
    half, packed = pieces[0].shape[1:]
    cols = latent + rope
    wide = latent + 128
    n = len(pieces)
    each = width // N_CTX
    room = -(-each // 16) * 16
    f32, bf16 = jnp.float32, jnp.bfloat16
    lanes = packed - 2 * cols
    n_x = N_DP // 2

    def kernel(me_ref, *refs):
        piece_refs, refs = refs[:n], refs[n:]
        x_ref, near_ref, far_ref, lat_ref, rope_ref, v_ref, joined, total, placed, v_total = refs
        me = [me_ref[i] for i in range(4)]
        my_x, my_hi = me_ref[4], me_ref[5]
        zero_pad = jnp.zeros((half, wide - cols), bf16)
        values = jnp.zeros((half, lanes), f32)
        for i, places in enumerate(items):
            for j, (ahead, hi) in enumerate(places):
                dp = (my_hi ^ hi) * n_x + lax.rem(my_x + ahead, n_x)
                values += piece_refs[i][j, :, 2 * cols :].astype(f32)
                for side in range(2):
                    at = pl.ds(pl.multiple_of(dp * tokens + side * half, half), half)
                    lat = piece_refs[i][j, :, side * latent : (side + 1) * latent]
                    start = 2 * latent + side * rope
                    rot = piece_refs[i][j, :, start : start + rope]
                    joined[at, :latent] = lat
                    joined[at, latent:] = jnp.concatenate([rot, zero_pad], axis=1)
                    if i == 0 and j == 0:
                        lat_ref[side * half : (side + 1) * half] = lat
                        rope_ref[side * half : (side + 1) * half] = rot
        v_total[...] = values
        mine = v_total[pl.ds(pl.multiple_of((my_hi * n_x + my_x) * heads, heads), heads), :]
        value = lanes // v_ref.shape[0]
        for r in range(v_ref.shape[0]):
            v_ref[r] = mine[:, r * value : (r + 1) * value]
        total[...] = tn(x_ref[...].reshape(count * tokens, width), joined[...])
        for c in range(N_CTX):
            placed[c, :each] = total[c * each : (c + 1) * each]
            if room > each:
                placed[c, each:] = jnp.zeros((room - each, wide), f32)

        def slot_step(slot, carry):
            for core, ref in enumerate((near_ref, far_ref)):
                owner = owner_at(me, core, slot // 2, slot % 2)
                ref[slot] = placed[owner, :, :cols].astype(bf16)
            return carry

        lax.fori_loop(0, N_CTX // 2, slot_step, 0)

    shape = ((N_CTX // 2, room, cols), bf16)
    return call(
        kernel,
        [
            shape,
            shape,
            ((tokens, latent), bf16),
            ((tokens, rope), bf16),
            ((lanes * half // (N_DP * heads * 128), heads, 128), f32),
        ],
        1,
        (me, *pieces, layer_input),
        [
            pltpu.VMEM((count * tokens, wide), bf16),
            pltpu.VMEM((width, wide), f32),
            pltpu.VMEM((N_CTX, room, wide), f32),
            pltpu.VMEM((half, lanes), f32),
        ],
        1000,
    )


def body(layer_input, kv_latent, key_rope, q_latent, q_rope, saved_output, w_uv, d_out, blocks):
    wide, bf16 = jnp.float32, jnp.bfloat16
    latent, rope = kv_latent.shape[2], key_rope.shape[2]
    heads = q_latent.shape[2]
    n_z = lax.axis_size("z")
    me = jnp.stack(
        [jnp.int32(n_z)] + [lax.axis_index(a) for a in ("z", "ylo", "core", "x", "yhi")]
    )

    mine = pack_keys(kv_latent[0], key_rope[0])
    ahead, behind = mine, mine
    groups, items, group, places = [], [], [], []
    for k in range(n_z // 2 + 1):
        if k:
            behind = shifted(behind, "z", 1)
            if k < n_z // 2:
                ahead = shifted(ahead, "z", -1)
        at_z = sorted({k, (n_z - k) % n_z})
        here = jnp.stack([ahead, behind][: len(at_z)] if k < n_z // 2 else [behind])
        there = swapped(here, "ylo")
        group += [here, there]
        places += [(z, y) for y in range(2) for z in at_z]
        if k in (n_z // 4, n_z // 2):
            groups.append(jnp.concatenate(group, axis=0))
            items.append(places)
            group, places = [], []
    pieces = list(groups)
    for x in groups:
        pieces.append(swapped(x, "core"))
    items = [[(core, *place) for place in p] for core in range(2) for p in items]

    outputs = saved_output.reshape(-1, latent)
    queries, grads, delta = prepare(
        q_latent.reshape(-1, latent), q_rope.reshape(-1, rope), outputs, d_out[0], w_uv
    )
    values = value_parts(me, outputs, d_out[0])
    d_q, d_qr, near_dk, far_dk = attention(
        me, blocks, pieces, items, queries, grads, delta, values
    )
    there_dk = swapped(far_dk, "core")
    sums = {}
    at = 0
    for batch in batches():
        n = len(batch)
        mine, other = (
            near_dk[k : k + n].astype(wide) + there_dk[k : k + n].astype(wide)
            for k in (at, at + n)
        )
        other = other.astype(bf16)
        other = swapped(other, "ylo")
        part = mine + other.astype(wide)
        for k, z in enumerate(batch):
            sums[z] = part[k]
        at += 2 * n
    summed = ring_sum([sums[k] for k in range(n_z)], "z").astype(bf16)
    summed = jnp.stack([summed, swapped(summed, "yhi")])

    n_x = lax.axis_size("x")
    after, before = shifted(summed, "x", -1), shifted(summed, "x", 1)
    opposite = [shifted(before[:1], "x", 1), shifted(after[1:], "x", -1)]
    dp_pieces = [summed, after, before] + opposite
    dp_items = [[(k, hi) for hi in range(2)] for k in (0, 1, n_x - 1)] + [[(2, 0)], [(2, 1)]]
    near_part, far_part, d_lat, d_rope, grad_uv = down_part(
        me, dp_pieces, dp_items, layer_input, latent, rope, heads
    )
    parts = (near_part.astype(wide) + swapped(far_part, "core").astype(wide)).astype(bf16)
    parts = parts.reshape(n_z, 2, *parts.shape[1:])
    part = ring_sum([parts[k] for k in range(n_z)], "z")
    grad_down = part[0] + swapped(part[1].astype(bf16), "ylo").astype(wide)
    return (
        d_q.reshape(q_latent.shape),
        d_qr.reshape(q_rope.shape),
        d_lat[None],
        d_rope[None],
        grad_down[: layer_input.shape[2] // N_CTX],
        grad_uv.reshape(-1, w_uv.shape[1]),
    )


DP = ("yhi", "x")
CTX = ("z", "ylo", "core")


def solution(mesh):
    n_dp, n_ctx = mesh.shape["dp"], mesh.shape["ctx"]
    fine = Mesh(mesh.devices.reshape(2, n_dp // 2, n_ctx // 4, 2, 2), DP + CTX)
    in_specs = (
        P(None, CTX, DP),
        P(DP, CTX, None),
        P(DP, CTX, None),
        P(DP, CTX, None, None),
        P(DP, CTX, None, None),
        P(DP, CTX, None, None),
        P(),
        P(DP, CTX, None),
        P(),
    )
    out_specs = (
        P(DP, CTX, None, None),
        P(DP, CTX, None, None),
        P(DP, CTX, None),
        P(DP, CTX, None),
        P(DP + CTX, None),
        P(DP + CTX, None),
    )

    return jax.shard_map(body, mesh=fine, in_specs=in_specs, out_specs=out_specs, check_vma=False)
```

```python
import functools
import math

import jax
import jax.numpy as jnp
from jax import lax
from jax.experimental import pallas as pl
from jax.experimental.pallas import tpu as pltpu
from jax.sharding import Mesh, PartitionSpec as P


softmax_scale = 1.0 / math.sqrt(192.0)
log2e = 1.0 / math.log(2.0)
TILE = 256
FIRST = 6
N_DP = 8
N_CTX = 32


def nt(a, b):
    return lax.dot_general(a, b, (((1,), (1,)), ((), ())), preferred_element_type=jnp.float32)


def nn(a, b):
    return lax.dot_general(a, b, (((1,), (0,)), ((), ())), preferred_element_type=jnp.float32)


def tn(a, b):
    return lax.dot_general(a, b, (((0,), (0,)), ((), ())), preferred_element_type=jnp.float32)


def swapped(x, axis):
    return lax.ppermute(x, axis, [(0, 1), (1, 0)])


def shifted(x, axis, by):
    n = lax.axis_size(axis)
    return lax.ppermute(x, axis, [(i, (i + by) % n) for i in range(n)])


def ring_sum(parts, axis):
    n = lax.axis_size(axis)
    f32, bf16 = jnp.float32, jnp.bfloat16
    up, down = (parts[k].astype(bf16) for k in (n // 2, n // 2 + 1))
    for k in range(n // 2 - 1, -1, -1):
        if k:
            up = (parts[k].astype(f32) + shifted(up, axis, 1).astype(f32)).astype(bf16)
        if 0 < k < n // 2 - 1:
            down = (parts[n - k].astype(f32) + shifted(down, axis, -1).astype(f32)).astype(bf16)
    up, down = shifted(up, axis, 1), shifted(down, axis, -1)
    return parts[0].astype(f32) + up.astype(f32) + down.astype(f32)


def owner_at(me, core, ahead, y):
    n_z, my_z, my_y, my_core = me[0], me[1], me[2], me[3]
    return (lax.rem(my_z + ahead, n_z) * 2 + (my_y ^ y)) * 2 + (my_core ^ core)


def batches():
    n = N_CTX // 4
    far = [[n // 2]] + [[k, n - k] for k in range(n // 2 - 1, 0, -1)]
    return far + [[0]]


def fill_owners(table, me):
    places = [(z, y) for batch in batches() for y in range(2) for z in batch]
    for core in range(2):
        for i, place in enumerate(places):
            table[core * len(places) + i] = owner_at(me, core, *place)


vmem = pl.BlockSpec(memory_space=pltpu.VMEM)
smem = pl.BlockSpec(memory_space=pltpu.SMEM)


def call(kernel, out_shape, n_smem, operands, scratch, flops, limit=60):
    return pl.pallas_call(
        kernel,
        out_shape=tuple(jax.ShapeDtypeStruct(*o) for o in out_shape),
        in_specs=[smem] * n_smem + [vmem] * (len(operands) - n_smem),
        out_specs=(vmem,) * len(out_shape),
        scratch_shapes=scratch,
        compiler_params=pltpu.CompilerParams(vmem_limit_bytes=limit * 1024 * 1024),
        cost_estimate=pl.CostEstimate(flops=flops, bytes_accessed=4 << 20, transcendentals=0),
    )(*operands)


def pack_keys(lat, rope):
    tokens, latent = lat.shape
    half, width = tokens // 2, rope.shape[1]

    def kernel(lat_ref, rope_ref, out_ref):
        out_ref[:, :latent] = lat_ref[:half]
        out_ref[:, latent : 2 * latent] = lat_ref[half:]
        out_ref[:, 2 * latent :] = jnp.concatenate([rope_ref[:half], rope_ref[half:]], axis=1)

    shape = ((half, 2 * (latent + width)), lat.dtype)
    return call(kernel, [shape], 0, (lat, rope), [], 1000, 8)[0]


def prepare(queries, query_rope, outputs, grad_out, weight):
    rows, latent = queries.shape
    rope = query_rope.shape[1]
    tokens = grad_out.shape[0]
    heads = rows // tokens
    value = grad_out.shape[1] // heads
    wide = latent + 128
    f32, bf16 = jnp.float32, jnp.bfloat16
    lanes = [slice(k, k + 128) for k in range(0, latent, 128)]

    def kernel(q_ref, qr_ref, out_ref, d_ref, w_ref, wide_ref, g_ref, delta_ref, g_wide):
        wide_ref[:, :latent] = q_ref[...]
        wide_ref[:, latent:] = jnp.concatenate(
            [qr_ref[...], jnp.zeros((rows, wide - latent - rope), bf16)], axis=1
        )

        def head_step(h, carry):
            column = pl.ds(pl.multiple_of(h * value, value), value)
            g = nt(d_ref[:, column], w_ref[:, column])
            for k, lane in enumerate(lanes):
                g_wide[k, pl.ds(h, tokens, stride=heads), :] = g[:, lane]
            return carry

        lax.fori_loop(0, heads, head_step, 0)
        delta = jnp.zeros((rows, 128), f32)
        for k, lane in enumerate(lanes):
            g = g_wide[k].astype(bf16)
            g_ref[:, lane] = g
            delta += g.astype(f32) * out_ref[:, lane].astype(f32)
        delta = jnp.sum(delta, axis=1, keepdims=True)
        delta = jnp.broadcast_to(delta, (rows, 128)).T[:1]
        delta_ref[0] = delta[:, : rows // 2]
        delta_ref[1] = delta[:, rows // 2 :]

    return call(
        kernel,
        [((rows, wide), bf16), ((rows, latent), bf16), ((2, 1, rows // 2), f32)],
        0,
        (queries, query_rope, outputs, grad_out, weight),
        [pltpu.VMEM((latent // 128, rows, 128), f32)],
        1000,
    )


def value_parts(me, outputs, grad_out):
    rows, latent = outputs.shape
    tokens = grad_out.shape[0]
    heads = rows // tokens
    value = grad_out.shape[1] // heads
    f32, bf16 = jnp.float32, jnp.bfloat16
    lanes = [slice(k, k + 128) for k in range(0, latent, 128)]
    n_dp = N_DP
    each = latent // (n_dp * N_CTX)

    def kernel(me_ref, out_ref, d_ref, v_ref, out_wide, v_wide, table):
        fill_owners(table, [me_ref[i] for i in range(4)])
        for k, lane in enumerate(lanes):
            out_wide[k] = out_ref[:, lane].astype(f32)

        def head_step(h, carry):
            d = d_ref[:, pl.ds(pl.multiple_of(h * value, value), value)]
            for k in range(len(lanes)):
                out = out_wide[k, pl.ds(h, tokens, stride=heads), :].astype(bf16)
                v_wide[pl.ds(h + k * 128 * heads, 128, stride=heads), :] = tn(out, d)
            return carry

        lax.fori_loop(0, heads, head_step, 0)

        def slot_step(slot, carry):
            owner = table[slot]
            for r in range(each):
                parts = []
                for dp in range(n_dp):
                    row = ((dp * N_CTX + owner) * each + r) * heads
                    parts.append(v_wide[pl.ds(pl.multiple_of(row, heads), heads), :])
                v_ref[slot, :, r * value : (r + 1) * value] = jnp.concatenate(
                    parts, axis=0
                ).astype(bf16)
            return carry

        lax.fori_loop(0, N_CTX, slot_step, 0)

    return call(
        kernel,
        [((N_CTX, n_dp * heads, each * value), bf16)],
        1,
        (me, outputs, grad_out),
        [
            pltpu.VMEM((latent // 128, rows, 128), f32),
            pltpu.VMEM((latent * heads, value), f32),
            pltpu.SMEM((N_CTX,), jnp.int32),
        ],
        1000,
    )[0]


def attention(me, blocks, pieces, items, queries, grads, delta, values):
    half, packed = pieces[0].shape[1:]
    rows, latent = grads.shape
    wide = queries.shape[1]
    cols = packed // 2
    rope = cols - latent
    count = 2 * N_CTX
    seq = count * half
    per, group = TILE // half, rows // 2
    heads = group // half
    f32, bf16 = jnp.float32, jnp.bfloat16
    n = len(pieces)
    extra = values.shape[2]
    n_z = N_CTX // 4

    def kernel(me_ref, blocks_ref, *refs):
        piece_refs, refs = refs[:n], refs[n:]
        q_ref, g_ref, delta_ref, v_ref, dq_ref, dqr_ref, near_ref, first_ref, rest_ref, *refs = refs
        keys_ref, table, scores, dk_acc, dq_acc = refs
        me = [me_ref[i] for i in range(4)]
        zero_pad = jnp.zeros((half, wide - cols), bf16)
        first = 0
        for ref, places in zip(piece_refs, items):
            for j, place in enumerate(places):
                table[first + j] = owner_at(me, *place)

            def sort_step(j, carry, ref=ref, first=first):
                owner = table[first + j]
                for side in range(2):
                    row = blocks_ref[2 * owner + side] * half
                    at = pl.ds(pl.multiple_of(row, half), half)
                    keys_ref[at, :latent] = ref[j, :, side * latent : (side + 1) * latent]
                    start = 2 * latent + side * rope
                    keys_ref[at, latent:] = jnp.concatenate(
                        [ref[j, :, start : start + rope], zero_pad], axis=1
                    )
                return carry

            lax.fori_loop(0, len(places), sort_step, 0)
            first += len(places)

        device = owner_at(me, 0, 0, 0)
        swap = (blocks_ref[2 * device + 1] > blocks_ref[2 * device]).astype(jnp.int32)
        top = jnp.maximum(blocks_ref[2 * device + 1], blocks_ref[2 * device]) // per

        def block_step(turn, carry):
            which = turn ^ swap
            block = blocks_ref[2 * device + which]
            base = pl.multiple_of(which * group, group)
            final = block // per

            def score_tile(t):
                at = pl.ds(pl.multiple_of(t * TILE, TILE), TILE)
                s = nt(keys_ref[at, :], q_ref[pl.ds(base, group), :])
                return s * (softmax_scale * log2e)

            def fold(t, s, m, l):
                scores[pl.ds(pl.multiple_of(t * TILE, TILE), TILE), :] = s
                new = jnp.maximum(m, jnp.max(s, axis=0, keepdims=True))
                l = l * jnp.exp2(m - new) + jnp.sum(jnp.exp2(s - new), axis=0, keepdims=True)
                return new, l

            begin = (jnp.full((1, group), -jnp.inf, f32), jnp.zeros((1, group), f32))
            m, l = lax.fori_loop(0, final, lambda t, c: fold(t, score_tile(t), *c), begin)
            ahead = block * half + lax.broadcasted_iota(jnp.int32, (1, group), 1) // heads
            row = lax.broadcasted_iota(jnp.int32, (TILE, group), 0)
            s = jnp.where(row <= ahead - final * TILE, score_tile(final), -jnp.inf)
            m, l = fold(final, s, m, l)
            log_total = m + jnp.log2(l)
            row_delta = delta_ref[which]
            dq_acc[...] = jnp.zeros((wide, group), f32)

            def tile_step(t, carry):
                at = pl.ds(pl.multiple_of(t * TILE, TILE), TILE)
                g = g_ref[pl.ds(base, group), :]
                p = jnp.exp2(scores[at, :] - log_total)
                dp = nt(keys_ref[at, :latent], g)
                ds = (p * (softmax_scale * (dp - row_delta))).astype(bf16)
                dk = nn(ds, q_ref[pl.ds(base, group), :])
                before = jnp.where(turn == 0, 0.0, dk_acc[at, :])
                dk_acc[at, :latent] = (
                    before[:, :latent] + dk[:, :latent] + nn(p.astype(bf16), g)
                )
                dk_acc[at, latent:] = before[:, latent:] + dk[:, latent:]
                dq_acc[...] += tn(keys_ref[at, :], ds)
                return carry

            lax.fori_loop(0, final + 1, tile_step, 0)
            done = dq_acc[...].T.astype(bf16)
            dq_ref[pl.ds(base, group), :] = done[:, :latent]
            dqr_ref[pl.ds(base, group), :] = done[:, latent:cols]
            return carry

        lax.fori_loop(0, 2, block_step, 0)
        fill_owners(table, me)

        def unsort_step(j, carry, far_ref, start):
            for core, out, k in ((0, near_ref, j), (1, far_ref, j - start)):
                owner = table[core * 2 * n_z + j]
                for side in range(2):
                    place = blocks_ref[2 * owner + side]
                    at = pl.ds(pl.multiple_of(place * half, half), half)
                    part = jnp.where(place // per <= top, dk_acc[at, :], 0.0).astype(bf16)
                    out[k, :, side * latent : (side + 1) * latent] = part[:, :latent]
                    column = 2 * latent + side * rope
                    out[k, :, column : column + rope] = part[:, latent:cols]
                out[k, :, packed:] = v_ref[core * 2 * n_z + j]
            return carry

        for far_ref, start, stop in ((first_ref, 0, FIRST), (rest_ref, FIRST, 2 * n_z)):
            lax.fori_loop(
                start, stop, functools.partial(unsort_step, far_ref=far_ref, start=start), 0
            )

    dk_shapes = [((k, half, packed + extra), bf16) for k in (2 * n_z, FIRST, 2 * n_z - FIRST)]
    return call(
        kernel,
        [((rows, latent), bf16), ((rows, rope), bf16), *dk_shapes],
        2,
        (me, blocks, *pieces, queries, grads, delta, values),
        [
            pltpu.VMEM((seq, wide), bf16),
            pltpu.SMEM((N_CTX,), jnp.int32),
            pltpu.VMEM((seq, group), f32),
            pltpu.VMEM((seq, wide), f32),
            pltpu.VMEM((wide, group), f32),
        ],
        5 * rows * seq * wide,
    )


def down_part(me, pieces, items, layer_input, latent, rope, heads):
    count, tokens, width = layer_input.shape
    half, packed = pieces[0].shape[1:]
    cols = latent + rope
    wide = latent + 128
    n = len(pieces)
    each = width // N_CTX
    room = -(-each // 16) * 16
    n_z = N_CTX // 4
    f32, bf16 = jnp.float32, jnp.bfloat16
    lanes = packed - 2 * cols
    n_x = N_DP // 2

    def kernel(me_ref, *refs):
        piece_refs, refs = refs[:n], refs[n:]
        x_ref, near_ref, far_ref, lat_ref, rope_ref, v_ref, joined, total, placed, v_total = refs
        me = [me_ref[i] for i in range(4)]
        my_x, my_hi = me_ref[4], me_ref[5]
        zero_pad = jnp.zeros((half, wide - cols), bf16)
        values = jnp.zeros((half, lanes), f32)
        for i, places in enumerate(items):
            for j, (ahead, hi) in enumerate(places):
                dp = (my_hi ^ hi) * n_x + lax.rem(my_x + ahead, n_x)
                values += piece_refs[i][j, :, 2 * cols :].astype(f32)
                for side in range(2):
                    at = pl.ds(pl.multiple_of(dp * tokens + side * half, half), half)
                    lat = piece_refs[i][j, :, side * latent : (side + 1) * latent]
                    start = 2 * latent + side * rope
                    rot = piece_refs[i][j, :, start : start + rope]
                    joined[at, :latent] = lat
                    joined[at, latent:] = jnp.concatenate([rot, zero_pad], axis=1)
                    if i == 0 and j == 0:
                        lat_ref[side * half : (side + 1) * half] = lat
                        rope_ref[side * half : (side + 1) * half] = rot
        v_total[...] = values
        mine = v_total[pl.ds(pl.multiple_of((my_hi * n_x + my_x) * heads, heads), heads), :]
        value = lanes // v_ref.shape[0]
        for r in range(v_ref.shape[0]):
            v_ref[r] = mine[:, r * value : (r + 1) * value]
        total[...] = tn(x_ref[...].reshape(count * tokens, width), joined[...])
        for c in range(N_CTX):
            placed[c, :each] = total[c * each : (c + 1) * each]
            if room > each:
                placed[c, each:] = jnp.zeros((room - each, wide), f32)

        def slot_step(slot, carry):
            for core, ref in enumerate((near_ref, far_ref)):
                owner = owner_at(me, core, lax.rem(slot, n_z), slot // n_z)
                ref[slot] = placed[owner, :, :cols].astype(bf16)
            return carry

        lax.fori_loop(0, N_CTX // 2, slot_step, 0)

    shape = ((N_CTX // 2, room, cols), bf16)
    return call(
        kernel,
        [
            shape,
            shape,
            ((tokens, latent), bf16),
            ((tokens, rope), bf16),
            ((lanes * half // (N_DP * heads * 128), heads, 128), f32),
        ],
        1,
        (me, *pieces, layer_input),
        [
            pltpu.VMEM((count * tokens, wide), bf16),
            pltpu.VMEM((width, wide), f32),
            pltpu.VMEM((N_CTX, room, wide), f32),
            pltpu.VMEM((half, lanes), f32),
        ],
        1000,
    )


def body(layer_input, kv_latent, key_rope, q_latent, q_rope, saved_output, w_uv, d_out, blocks):
    wide, bf16 = jnp.float32, jnp.bfloat16
    latent, rope = kv_latent.shape[2], key_rope.shape[2]
    heads = q_latent.shape[2]
    n_z = lax.axis_size("z")
    me = jnp.stack(
        [jnp.int32(n_z)] + [lax.axis_index(a) for a in ("z", "ylo", "core", "x", "yhi")]
    )

    mine = pack_keys(kv_latent[0], key_rope[0])
    ahead, behind = mine, mine
    groups, items, group, places = [], [], [], []
    for k in range(n_z // 2 + 1):
        if k:
            behind = shifted(behind, "z", 1)
            if k < n_z // 2:
                ahead = shifted(ahead, "z", -1)
        at_z = sorted({k, (n_z - k) % n_z})
        here = jnp.stack([ahead, behind][: len(at_z)] if k < n_z // 2 else [behind])
        there = swapped(here, "ylo")
        group += [here, there]
        places += [(z, y) for y in range(2) for z in at_z]
        if k in (n_z // 4, n_z // 2):
            groups.append(jnp.concatenate(group, axis=0))
            items.append(places)
            group, places = [], []
    pieces = list(groups)
    for x in groups:
        pieces.append(swapped(x, "core"))
    items = [[(core, *place) for place in p] for core in range(2) for p in items]

    outputs = saved_output.reshape(-1, latent)
    queries, grads, delta = prepare(
        q_latent.reshape(-1, latent), q_rope.reshape(-1, rope), outputs, d_out[0], w_uv
    )
    values = value_parts(me, outputs, d_out[0])
    d_q, d_qr, near_dk, *far_dk = attention(
        me, blocks, pieces, items, queries, grads, delta, values
    )
    first_dk = swapped(far_dk[0], "core")
    rest_dk = swapped(far_dk[1], "core")
    sums, sent = {}, []
    at = 0
    for i, batch in enumerate(batches()):
        n = len(batch)
        if at == FIRST:
            rest_dk, *_ = lax.optimization_barrier((rest_dk, *sent))
        there_dk, start = (first_dk, at) if at < FIRST else (rest_dk, at - FIRST)
        mine, other = (
            near_dk[at + k : at + k + n].astype(wide)
            + there_dk[start + k : start + k + n].astype(wide)
            for k in (0, n)
        )
        sent.append(other.astype(bf16))
        part = mine + swapped(sent[i], "ylo").astype(wide)
        for k, z in enumerate(batch):
            sums[z] = part[k]
        at += 2 * n
    summed = ring_sum([sums[k] for k in range(n_z)], "z").astype(bf16)
    summed = jnp.stack([summed, swapped(summed, "yhi")])

    n_x = lax.axis_size("x")
    after, before = shifted(summed, "x", -1), shifted(summed, "x", 1)
    opposite = [shifted(before[:1], "x", 1), shifted(after[1:], "x", -1)]
    dp_pieces = [summed, after, before] + opposite
    dp_items = [[(k, hi) for hi in range(2)] for k in (0, 1, n_x - 1)] + [[(2, 0)], [(2, 1)]]
    near_part, far_part, d_lat, d_rope, grad_uv = down_part(
        me, dp_pieces, dp_items, layer_input, latent, rope, heads
    )
    there_part = swapped(far_part, "core")
    mine, other = (
        near_part[k : k + n_z].astype(wide) + there_part[k : k + n_z].astype(wide)
        for k in (0, n_z)
    )
    parts = mine + swapped(other.astype(bf16), "ylo").astype(wide)
    grad_down = parts[0]
    for k in range(1, n_z):
        grad_down = grad_down + shifted(parts[k].astype(bf16), "z", k).astype(wide)
    return (
        d_q.reshape(q_latent.shape),
        d_qr.reshape(q_rope.shape),
        d_lat[None],
        d_rope[None],
        grad_down[: layer_input.shape[2] // N_CTX],
        grad_uv.reshape(-1, w_uv.shape[1]),
    )


DP = ("yhi", "x")
CTX = ("z", "ylo", "core")


def solution(mesh):
    n_dp, n_ctx = mesh.shape["dp"], mesh.shape["ctx"]
    fine = Mesh(mesh.devices.reshape(2, n_dp // 2, n_ctx // 4, 2, 2), DP + CTX)
    in_specs = (
        P(None, CTX, DP),
        P(DP, CTX, None),
        P(DP, CTX, None),
        P(DP, CTX, None, None),
        P(DP, CTX, None, None),
        P(DP, CTX, None, None),
        P(),
        P(DP, CTX, None),
        P(),
    )
    out_specs = (
        P(DP, CTX, None, None),
        P(DP, CTX, None, None),
        P(DP, CTX, None),
        P(DP, CTX, None),
        P(DP + CTX, None),
        P(DP + CTX, None),
    )

    return jax.shard_map(body, mesh=fine, in_specs=in_specs, out_specs=out_specs, check_vma=False)
```

```python
import functools
import math

import jax
import jax.numpy as jnp
from jax import lax
from jax.experimental import pallas as pl
from jax.experimental.pallas import tpu as pltpu
from jax.sharding import Mesh, PartitionSpec as P


softmax_scale = 1.0 / math.sqrt(192.0)
log2e = 1.0 / math.log(2.0)
TILE = 256
FIRST = 6
N_DP = 8
N_CTX = 32


def nt(a, b):
    return lax.dot_general(a, b, (((1,), (1,)), ((), ())), preferred_element_type=jnp.float32)


def nn(a, b):
    return lax.dot_general(a, b, (((1,), (0,)), ((), ())), preferred_element_type=jnp.float32)


def tn(a, b):
    return lax.dot_general(a, b, (((0,), (0,)), ((), ())), preferred_element_type=jnp.float32)


def swapped(x, axis):
    return lax.ppermute(x, axis, [(0, 1), (1, 0)])


def shifted(x, axis, by):
    n = lax.axis_size(axis)
    return lax.ppermute(x, axis, [(i, (i + by) % n) for i in range(n)])


def ring_sum(parts, axis):
    n = lax.axis_size(axis)
    f32, bf16 = jnp.float32, jnp.bfloat16
    up, down = (parts[k].astype(bf16) for k in (n // 2, n // 2 + 1))
    for k in range(n // 2 - 1, -1, -1):
        if k:
            up = (parts[k].astype(f32) + shifted(up, axis, 1).astype(f32)).astype(bf16)
        if 0 < k < n // 2 - 1:
            down = (parts[n - k].astype(f32) + shifted(down, axis, -1).astype(f32)).astype(bf16)
    up, down = shifted(up, axis, 1), shifted(down, axis, -1)
    return parts[0].astype(f32) + up.astype(f32) + down.astype(f32)


def owner_at(me, core, ahead, y):
    n_z, my_z, my_y, my_core = me[0], me[1], me[2], me[3]
    return (lax.rem(my_z + ahead, n_z) * 2 + (my_y ^ y)) * 2 + (my_core ^ core)


def batches():
    n = N_CTX // 4
    far = [[n // 2]] + [[k, n - k] for k in range(n // 2 - 1, 0, -1)]
    return far + [[0]]


def fill_owners(table, me):
    places = [(z, y) for batch in batches() for y in range(2) for z in batch]
    for core in range(2):
        for i, place in enumerate(places):
            table[core * len(places) + i] = owner_at(me, core, *place)


vmem = pl.BlockSpec(memory_space=pltpu.VMEM)
smem = pl.BlockSpec(memory_space=pltpu.SMEM)


def call(kernel, out_shape, n_smem, operands, scratch, flops, limit=60):
    return pl.pallas_call(
        kernel,
        out_shape=tuple(jax.ShapeDtypeStruct(*o) for o in out_shape),
        in_specs=[smem] * n_smem + [vmem] * (len(operands) - n_smem),
        out_specs=(vmem,) * len(out_shape),
        scratch_shapes=scratch,
        compiler_params=pltpu.CompilerParams(vmem_limit_bytes=limit * 1024 * 1024),
        cost_estimate=pl.CostEstimate(flops=flops, bytes_accessed=4 << 20, transcendentals=0),
    )(*operands)


def pack_keys(lat, rope):
    tokens, latent = lat.shape
    half, width = tokens // 2, rope.shape[1]

    def kernel(lat_ref, rope_ref, out_ref):
        out_ref[:, :latent] = lat_ref[:half]
        out_ref[:, latent : 2 * latent] = lat_ref[half:]
        out_ref[:, 2 * latent :] = jnp.concatenate([rope_ref[:half], rope_ref[half:]], axis=1)

    shape = ((half, 2 * (latent + width)), lat.dtype)
    return call(kernel, [shape], 0, (lat, rope), [], 1000, 8)[0]


def prepare(queries, query_rope, outputs, grad_out, weight):
    rows, latent = queries.shape
    rope = query_rope.shape[1]
    tokens = grad_out.shape[0]
    heads = rows // tokens
    value = grad_out.shape[1] // heads
    wide = latent + 128
    f32, bf16 = jnp.float32, jnp.bfloat16
    lanes = [slice(k, k + 128) for k in range(0, latent, 128)]

    def kernel(q_ref, qr_ref, out_ref, d_ref, w_ref, wide_ref, g_ref, delta_ref, g_wide):
        wide_ref[:, :latent] = q_ref[...]
        wide_ref[:, latent:] = jnp.concatenate(
            [qr_ref[...], jnp.zeros((rows, wide - latent - rope), bf16)], axis=1
        )

        def head_step(h, carry):
            column = pl.ds(pl.multiple_of(h * value, value), value)
            g = nt(d_ref[:, column], w_ref[:, column])
            for k, lane in enumerate(lanes):
                g_wide[k, pl.ds(h, tokens, stride=heads), :] = g[:, lane]
            return carry

        lax.fori_loop(0, heads, head_step, 0)
        delta = jnp.zeros((rows, 128), f32)
        for k, lane in enumerate(lanes):
            g = g_wide[k].astype(bf16)
            g_ref[:, lane] = g
            delta += g.astype(f32) * out_ref[:, lane].astype(f32)
        delta = jnp.sum(delta, axis=1, keepdims=True)
        delta = jnp.broadcast_to(delta, (rows, 128)).T[:1]
        delta_ref[0] = delta[:, : rows // 2]
        delta_ref[1] = delta[:, rows // 2 :]

    return call(
        kernel,
        [((rows, wide), bf16), ((rows, latent), bf16), ((2, 1, rows // 2), f32)],
        0,
        (queries, query_rope, outputs, grad_out, weight),
        [pltpu.VMEM((latent // 128, rows, 128), f32)],
        1000,
    )


def value_parts(me, outputs, grad_out):
    rows, latent = outputs.shape
    tokens = grad_out.shape[0]
    heads = rows // tokens
    value = grad_out.shape[1] // heads
    f32, bf16 = jnp.float32, jnp.bfloat16
    lanes = [slice(k, k + 128) for k in range(0, latent, 128)]
    n_dp = N_DP
    each = latent // (n_dp * N_CTX)

    def kernel(me_ref, out_ref, d_ref, v_ref, out_wide, v_wide, table):
        fill_owners(table, [me_ref[i] for i in range(4)])
        for k, lane in enumerate(lanes):
            out_wide[k] = out_ref[:, lane].astype(f32)

        def head_step(h, carry):
            d = d_ref[:, pl.ds(pl.multiple_of(h * value, value), value)]
            for k in range(len(lanes)):
                out = out_wide[k, pl.ds(h, tokens, stride=heads), :].astype(bf16)
                v_wide[pl.ds(h + k * 128 * heads, 128, stride=heads), :] = tn(out, d)
            return carry

        lax.fori_loop(0, heads, head_step, 0)

        def slot_step(slot, carry):
            owner = table[slot]
            for r in range(each):
                parts = []
                for dp in range(n_dp):
                    row = ((dp * N_CTX + owner) * each + r) * heads
                    parts.append(v_wide[pl.ds(pl.multiple_of(row, heads), heads), :])
                v_ref[slot, :, r * value : (r + 1) * value] = jnp.concatenate(
                    parts, axis=0
                ).astype(bf16)
            return carry

        lax.fori_loop(0, N_CTX, slot_step, 0)

    return call(
        kernel,
        [((N_CTX, n_dp * heads, each * value), bf16)],
        1,
        (me, outputs, grad_out),
        [
            pltpu.VMEM((latent // 128, rows, 128), f32),
            pltpu.VMEM((latent * heads, value), f32),
            pltpu.SMEM((N_CTX,), jnp.int32),
        ],
        1000,
    )[0]


def attention(me, blocks, pieces, items, queries, grads, delta, values):
    half, packed = pieces[0].shape[1:]
    rows, latent = grads.shape
    wide = queries.shape[1]
    cols = packed // 2
    rope = cols - latent
    count = 2 * N_CTX
    seq = count * half
    per, group = TILE // half, rows // 2
    heads = group // half
    f32, bf16 = jnp.float32, jnp.bfloat16
    n = len(pieces)
    extra = values.shape[2]
    n_z = N_CTX // 4

    def kernel(me_ref, blocks_ref, *refs):
        piece_refs, refs = refs[:n], refs[n:]
        q_ref, g_ref, delta_ref, v_ref, dq_ref, dqr_ref, near_ref, first_ref, rest_ref, *refs = refs
        keys_ref, table, scores, dk_acc, dq_acc = refs
        me = [me_ref[i] for i in range(4)]
        zero_pad = jnp.zeros((half, wide - cols), bf16)
        first = 0
        for ref, places in zip(piece_refs, items):
            for j, place in enumerate(places):
                table[first + j] = owner_at(me, *place)

            def sort_step(j, carry, ref=ref, first=first):
                owner = table[first + j]
                for side in range(2):
                    row = blocks_ref[2 * owner + side] * half
                    at = pl.ds(pl.multiple_of(row, half), half)
                    keys_ref[at, :latent] = ref[j, :, side * latent : (side + 1) * latent]
                    start = 2 * latent + side * rope
                    keys_ref[at, latent:] = jnp.concatenate(
                        [ref[j, :, start : start + rope], zero_pad], axis=1
                    )
                return carry

            lax.fori_loop(0, len(places), sort_step, 0)
            first += len(places)

        device = owner_at(me, 0, 0, 0)
        swap = (blocks_ref[2 * device + 1] > blocks_ref[2 * device]).astype(jnp.int32)
        top = jnp.maximum(blocks_ref[2 * device + 1], blocks_ref[2 * device]) // per

        def block_step(turn, carry):
            which = turn ^ swap
            block = blocks_ref[2 * device + which]
            base = pl.multiple_of(which * group, group)
            final = block // per

            def score_tile(t):
                at = pl.ds(pl.multiple_of(t * TILE, TILE), TILE)
                s = nt(keys_ref[at, :], q_ref[pl.ds(base, group), :])
                return s * (softmax_scale * log2e)

            def fold(t, s, m, l):
                scores[pl.ds(pl.multiple_of(t * TILE, TILE), TILE), :] = s
                new = jnp.maximum(m, jnp.max(s, axis=0, keepdims=True))
                l = l * jnp.exp2(m - new) + jnp.sum(jnp.exp2(s - new), axis=0, keepdims=True)
                return new, l

            begin = (jnp.full((1, group), -jnp.inf, f32), jnp.zeros((1, group), f32))
            m, l = lax.fori_loop(0, final, lambda t, c: fold(t, score_tile(t), *c), begin)
            ahead = block * half + lax.broadcasted_iota(jnp.int32, (1, group), 1) // heads
            row = lax.broadcasted_iota(jnp.int32, (TILE, group), 0)
            s = jnp.where(row <= ahead - final * TILE, score_tile(final), -jnp.inf)
            m, l = fold(final, s, m, l)
            log_total = m + jnp.log2(l)
            row_delta = delta_ref[which]
            dq_acc[...] = jnp.zeros((wide, group), f32)

            def tile_step(t, carry):
                at = pl.ds(pl.multiple_of(t * TILE, TILE), TILE)
                g = g_ref[pl.ds(base, group), :]
                p = jnp.exp2(scores[at, :] - log_total)
                dp = nt(keys_ref[at, :latent], g)
                ds = (p * (softmax_scale * (dp - row_delta))).astype(bf16)
                dk = nn(ds, q_ref[pl.ds(base, group), :])
                before = jnp.where(turn == 0, 0.0, dk_acc[at, :])
                dk_acc[at, :latent] = (
                    before[:, :latent] + dk[:, :latent] + nn(p.astype(bf16), g)
                )
                dk_acc[at, latent:] = before[:, latent:] + dk[:, latent:]
                dq_acc[...] += tn(keys_ref[at, :], ds)
                return carry

            lax.fori_loop(0, final + 1, tile_step, 0)
            done = dq_acc[...].T.astype(bf16)
            dq_ref[pl.ds(base, group), :] = done[:, :latent]
            dqr_ref[pl.ds(base, group), :] = done[:, latent:cols]
            return carry

        lax.fori_loop(0, 2, block_step, 0)
        fill_owners(table, me)

        def unsort_step(j, carry, far_ref, start):
            for core, out, k in ((0, near_ref, j), (1, far_ref, j - start)):
                owner = table[core * 2 * n_z + j]
                for side in range(2):
                    place = blocks_ref[2 * owner + side]
                    at = pl.ds(pl.multiple_of(place * half, half), half)
                    part = jnp.where(place // per <= top, dk_acc[at, :], 0.0).astype(bf16)
                    out[k, :, side * latent : (side + 1) * latent] = part[:, :latent]
                    column = 2 * latent + side * rope
                    out[k, :, column : column + rope] = part[:, latent:cols]
                out[k, :, packed:] = v_ref[core * 2 * n_z + j]
            return carry

        for far_ref, start, stop in ((first_ref, 0, FIRST), (rest_ref, FIRST, 2 * n_z)):
            lax.fori_loop(
                start, stop, functools.partial(unsort_step, far_ref=far_ref, start=start), 0
            )

    dk_shapes = [((k, half, packed + extra), bf16) for k in (2 * n_z, FIRST, 2 * n_z - FIRST)]
    return call(
        kernel,
        [((rows, latent), bf16), ((rows, rope), bf16), *dk_shapes],
        2,
        (me, blocks, *pieces, queries, grads, delta, values),
        [
            pltpu.VMEM((seq, wide), bf16),
            pltpu.SMEM((N_CTX,), jnp.int32),
            pltpu.VMEM((seq, group), f32),
            pltpu.VMEM((seq, wide), f32),
            pltpu.VMEM((wide, group), f32),
        ],
        5 * rows * seq * wide,
    )


def down_part(me, pieces, items, layer_input, latent, rope, heads):
    count, tokens, width = layer_input.shape
    half, packed = pieces[0].shape[1:]
    cols = latent + rope
    wide = latent + 128
    n = len(pieces)
    each = width // N_CTX
    room = -(-each // 16) * 16
    n_z = N_CTX // 4
    f32, bf16 = jnp.float32, jnp.bfloat16
    lanes = packed - 2 * cols
    n_x = N_DP // 2

    def kernel(me_ref, *refs):
        piece_refs, refs = refs[:n], refs[n:]
        x_ref, near_ref, far_ref, lat_ref, rope_ref, v_ref, joined, total, placed, v_total = refs
        me = [me_ref[i] for i in range(4)]
        my_x, my_hi = me_ref[4], me_ref[5]
        zero_pad = jnp.zeros((half, wide - cols), bf16)
        values = jnp.zeros((half, lanes), f32)
        for i, places in enumerate(items):
            for j, (ahead, hi) in enumerate(places):
                dp = (my_hi ^ hi) * n_x + lax.rem(my_x + ahead, n_x)
                values += piece_refs[i][j, :, 2 * cols :].astype(f32)
                for side in range(2):
                    at = pl.ds(pl.multiple_of(dp * tokens + side * half, half), half)
                    lat = piece_refs[i][j, :, side * latent : (side + 1) * latent]
                    start = 2 * latent + side * rope
                    rot = piece_refs[i][j, :, start : start + rope]
                    joined[at, :latent] = lat
                    joined[at, latent:] = jnp.concatenate([rot, zero_pad], axis=1)
                    if i == 0 and j == 0:
                        lat_ref[side * half : (side + 1) * half] = lat
                        rope_ref[side * half : (side + 1) * half] = rot
        v_total[...] = values
        mine = v_total[pl.ds(pl.multiple_of((my_hi * n_x + my_x) * heads, heads), heads), :]
        value = lanes // v_ref.shape[0]
        for r in range(v_ref.shape[0]):
            v_ref[r] = mine[:, r * value : (r + 1) * value]
        total[...] = tn(x_ref[...].reshape(count * tokens, width), joined[...])
        for c in range(N_CTX):
            placed[c, :each] = total[c * each : (c + 1) * each]
            if room > each:
                placed[c, each:] = jnp.zeros((room - each, wide), f32)

        def slot_step(slot, carry):
            for core, ref in enumerate((near_ref, far_ref)):
                owner = owner_at(me, core, lax.rem(slot + n_z // 4, n_z), slot // n_z)
                ref[slot] = placed[owner, :, :cols].astype(bf16)
            return carry

        lax.fori_loop(0, N_CTX // 2, slot_step, 0)

    shape = ((N_CTX // 2, room, cols), bf16)
    return call(
        kernel,
        [
            shape,
            shape,
            ((tokens, latent), bf16),
            ((tokens, rope), bf16),
            ((lanes * half // (N_DP * heads * 128), heads, 128), f32),
        ],
        1,
        (me, *pieces, layer_input),
        [
            pltpu.VMEM((count * tokens, wide), bf16),
            pltpu.VMEM((width, wide), f32),
            pltpu.VMEM((N_CTX, room, wide), f32),
            pltpu.VMEM((half, lanes), f32),
        ],
        1000,
    )


def body(layer_input, kv_latent, key_rope, q_latent, q_rope, saved_output, w_uv, d_out, blocks):
    wide, bf16 = jnp.float32, jnp.bfloat16
    latent, rope = kv_latent.shape[2], key_rope.shape[2]
    heads = q_latent.shape[2]
    n_z = lax.axis_size("z")
    me = jnp.stack(
        [jnp.int32(n_z)] + [lax.axis_index(a) for a in ("z", "ylo", "core", "x", "yhi")]
    )

    mine = pack_keys(kv_latent[0], key_rope[0])
    ahead, behind = mine, mine
    groups, items, group, places = [], [], [], []
    for k in range(n_z // 2 + 1):
        if k:
            behind = shifted(behind, "z", 1)
            if k < n_z // 2:
                ahead = shifted(ahead, "z", -1)
        at_z = sorted({k, (n_z - k) % n_z})
        here = jnp.stack([ahead, behind][: len(at_z)] if k < n_z // 2 else [behind])
        there = swapped(here, "ylo")
        group += [here, there]
        places += [(z, y) for y in range(2) for z in at_z]
        if k in (n_z // 4, n_z // 2):
            groups.append(jnp.concatenate(group, axis=0))
            items.append(places)
            group, places = [], []
    pieces = list(groups)
    for x in groups:
        pieces.append(swapped(x, "core"))
    items = [[(core, *place) for place in p] for core in range(2) for p in items]

    outputs = saved_output.reshape(-1, latent)
    queries, grads, delta = prepare(
        q_latent.reshape(-1, latent), q_rope.reshape(-1, rope), outputs, d_out[0], w_uv
    )
    values = value_parts(me, outputs, d_out[0])
    d_q, d_qr, near_dk, *far_dk = attention(
        me, blocks, pieces, items, queries, grads, delta, values
    )
    first_dk = swapped(far_dk[0], "core")
    rest_dk = swapped(far_dk[1], "core")
    sums, sent = {}, []
    at = 0
    for i, batch in enumerate(batches()):
        n = len(batch)
        if at == FIRST:
            rest_dk, *_ = lax.optimization_barrier((rest_dk, *sent))
        there_dk, start = (first_dk, at) if at < FIRST else (rest_dk, at - FIRST)
        mine, other = (
            near_dk[at + k : at + k + n].astype(wide)
            + there_dk[start + k : start + k + n].astype(wide)
            for k in (0, n)
        )
        sent.append(other.astype(bf16))
        part = mine + swapped(sent[i], "ylo").astype(wide)
        for k, z in enumerate(batch):
            sums[z] = part[k]
        at += 2 * n
    summed = ring_sum([sums[k] for k in range(n_z)], "z").astype(bf16)
    summed = jnp.stack([summed, swapped(summed, "yhi")])

    n_x = lax.axis_size("x")
    after, before = shifted(summed, "x", -1), shifted(summed, "x", 1)
    opposite = [shifted(before[:1], "x", 1), shifted(after[1:], "x", -1)]
    dp_pieces = [summed, after, before] + opposite
    dp_items = [[(k, hi) for hi in range(2)] for k in (0, 1, n_x - 1)] + [[(2, 0)], [(2, 1)]]
    near_part, far_part, d_lat, d_rope, grad_uv = down_part(
        me, dp_pieces, dp_items, layer_input, latent, rope, heads
    )
    there_part = swapped(far_part, "core")
    grad_down, far_parts = 0.0, None
    for start, stop in ((0, n_z // 2 + 1), (n_z // 2 + 1, n_z)):
        mine, other = (
            near_part[k + start : k + stop].astype(wide)
            + there_part[k + start : k + stop].astype(wide)
            for k in (0, n_z)
        )
        other = swapped(other.astype(bf16), "ylo")
        if far_parts is not None:
            other, _ = lax.optimization_barrier((other, far_parts))
        parts = mine + other.astype(wide)
        far_parts = parts.astype(bf16)
        for k in range(start, stop):
            z = (k + n_z // 4) % n_z
            part = shifted(far_parts[k - start], "z", z) if z else parts[k - start]
            grad_down = grad_down + part.astype(wide)
    grad_down = grad_down[: layer_input.shape[2] // N_CTX]
    return (
        d_q.reshape(q_latent.shape),
        d_qr.reshape(q_rope.shape),
        d_lat[None],
        d_rope[None],
        grad_down,
        grad_uv.reshape(-1, w_uv.shape[1]),
    )


DP = ("yhi", "x")
CTX = ("z", "ylo", "core")


def solution(mesh):
    n_dp, n_ctx = mesh.shape["dp"], mesh.shape["ctx"]
    fine = Mesh(mesh.devices.reshape(2, n_dp // 2, n_ctx // 4, 2, 2), DP + CTX)
    in_specs = (
        P(None, CTX, DP),
        P(DP, CTX, None),
        P(DP, CTX, None),
        P(DP, CTX, None, None),
        P(DP, CTX, None, None),
        P(DP, CTX, None, None),
        P(),
        P(DP, CTX, None),
        P(),
    )
    out_specs = (
        P(DP, CTX, None, None),
        P(DP, CTX, None, None),
        P(DP, CTX, None),
        P(DP, CTX, None),
        P(DP + CTX, None),
        P(DP + CTX, None),
    )

    return jax.shard_map(body, mesh=fine, in_specs=in_specs, out_specs=out_specs, check_vma=False)
```
